32 devices in a mesh: row: 4 (over y, x), col: 8 (over z, core).
Axes of the slice: x: 2, y: 2, z: 4, core: 2. Of those that a mesh axis runs over, the one named last changes fastest.
Arguments:
- depth: float32 [256, 4096], P('row', 'col'), may hold values from 0 to 1
- rainfall: float32 [256, 4096], P('row', 'col'), may hold values from 0.05 to 0.5
- conveyance: float32 [256, 4096], P('row', 'col'), may hold values from 0.2 to 5
- flow_dir: int32 [256, 4096], P('row', 'col'), may hold values from 0 to 7, as said below
- outlet: int32 [256, 4096], P('row', 'col'), may hold values 0 or 1
Outputs:
- new_depth: float32 [256, 4096], P('row', 'col')
- discharge: float32 [256, 4096], P('row', 'col')
The draws below stay inside these ranges and needn't reach their ends.
Inputs may be any that keep to these rules, and one draw needn't show every extreme that they name: `flow_dir`: each cell's code is 0 to 7.
All inputs are finite; a program needn't handle non-finite values. No bound on the sum of `outlet` on one device may be relied on, other than what follows from the above.
Results may differ from the reference program's by a relative error of at most 0.00002.
Values sent between devices are 32-bit elements; how exact they have to be, the bound alone decides.
A program may use at most 64 MiB of HBM per device.

```python
import math
import jax
import jax.numpy as jnp

SUBSTEPS = 3
PASSES = 64
NR = 256
NC = 4096


def draw_flow_dir(key, part):
    first = jax.random.fold_in(key, 11)
    second = jax.random.fold_in(key, 12)
    third = jax.random.fold_in(key, 13)
    picker = jax.random.randint(first, (NR, NC), 0, 10)
    drift = jax.random.randint(second, (NR, NC), 0, 3)
    anyway = jax.random.randint(third, (NR, NC), 0, 8)
    return jnp.where(picker < 7, drift, anyway).astype(jnp.int32)


def plant(array, key, low, top_value):
    longest = array.shape.index(max(array.shape))
    spots = []
    for shift in (0, 1):
        where = [jax.random.randint(jax.random.fold_in(key, axis), (), 0, length) for axis, length in enumerate(array.shape)]
        where[longest] = (where[longest] + shift) % array.shape[longest]
        spots.append(tuple(where))
    return array.at[spots[0]].set(low).at[spots[1]].set(top_value)


def levels(own_key, extent, split, low, largest):
    def one(axis_at, blocks):
        draws = jax.random.uniform(jax.random.fold_in(jax.random.fold_in(own_key, 6), axis_at), (blocks,), jnp.float32, low / len(split), largest / len(split))
        return jnp.repeat(jnp.exp(draws), extent[axis_at] // blocks).reshape((-1,) + (1,) * (len(extent) - axis_at - 1))

    gain = one(*split[0])
    for cut in split[1:]:
        gain = gain * one(*cut)
    return gain


def setup_inputs(seed: int = 0) -> dict:
    arg_keys = jax.random.split(jax.random.key(seed), 6)
    depth = jnp.clip(1.0 * jax.random.uniform(arg_keys[0], (NR, NC), jnp.float32) ** levels(arg_keys[0], (NR, NC), ((0, 4), (1, 8)), -0.2, 0.2), 0.0, 1.0)
    rainfall = jnp.clip(jnp.exp(math.log(0.5) - 2.3025851 * jax.random.uniform(arg_keys[1], (NR, NC), jnp.float32) ** levels(arg_keys[1], (NR, NC), ((0, 4), (1, 8)), -0.2, 0.2)), 0.05, 0.5)
    conveyance = jnp.clip(jnp.exp(math.log(5.0) - 3.218876 * jax.random.uniform(arg_keys[2], (NR, NC), jnp.float32) ** levels(arg_keys[2], (NR, NC), ((0, 4), (1, 8)), -0.2, 0.2)), 0.2, 5.0)
    flow_dir = draw_flow_dir(jax.random.fold_in(arg_keys[5], 71), 0)
    outlet = plant((jax.random.randint(arg_keys[4], (NR, NC), 0, 32) < 1).astype(jnp.int32), jax.random.fold_in(arg_keys[4], 1), 0, 1)
    return dict(depth=depth, rainfall=rainfall, conveyance=conveyance, flow_dir=flow_dir, outlet=outlet)


OFFSETS = ((0, 1), (1, 1), (1, 0), (1, -1), (0, -1), (-1, -1), (-1, 0), (-1, 1))


def inflow(sent, route):
    sent_pad = jnp.pad(sent, 1)
    route_pad = jnp.pad(route, 1)
    rows, cols = sent.shape
    total = jnp.zeros((rows, cols), jnp.float32)
    for k, (di, dj) in enumerate(OFFSETS):
        source = sent_pad[1 - di:1 - di + rows, 1 - dj:1 - dj + cols]
        target = route_pad[1 - di:1 - di + rows, 1 - dj:1 - dj + cols]
        total = total + jnp.where(target == k + 1, source, jnp.float32(0.0))
    return total


def reference(depth, rainfall, conveyance, flow_dir, outlet):
    route = jnp.where(outlet == 1, 0, flow_dir + 1).astype(jnp.int32)
    length = jnp.where(flow_dir % 2 == 1, jnp.float32(0.70710678), jnp.float32(1.0))
    level = depth
    for step in range(SUBSTEPS):
        factor = conveyance * length * jnp.power(level, jnp.float32(2.0 / 3.0))
        share = factor / (1.0 + factor)
        out = level * share
        sent = jnp.where(route > 0, out, jnp.float32(0.0))
        level = level + rainfall - out + inflow(sent, route)

    def one_pass(index, acc):
        sent = jnp.where(route > 0, acc, jnp.float32(0.0))
        return level + inflow(sent, route)

    acc = jax.lax.fori_loop(0, PASSES, one_pass, level)
    return level, jnp.log(1.0 + acc)
```

```python
import functools

import jax
import jax.numpy as jnp
from jax import lax
from jax.experimental import pallas as pl
from jax.experimental.pallas import tpu as pltpu
from jax.sharding import PartitionSpec as P

SUBSTEPS = 3
PASSES = 64
OFFSETS = ((0, 1), (1, 1), (1, 0), (1, -1), (0, -1), (-1, -1), (-1, 0), (-1, 1))
LANES = 128
SUB = 8
NEAR = 8
MARGIN = 32
GROUPS = PASSES // MARGIN
SPARE = 0
VMEM_BYTES = 40 * 1024 * 1024
MESH = pl.DeviceIdType.MESH


def kernel(
    row_peers, col_peers,
    depth_hbm, rain_hbm, conv_hbm, dir_hbm, outlet_hbm,
    out_ref,
    depth_ref, rain_ref, conv_ref, dir_ref, outlet_ref, load_sem,
    depth_ext, rain_ext, coef_ext, route_ext, far_ext, acc_ext, plain, pack_out, pack_in,
    acc, rain, coef, level, share, masks,
    send_sem, recv_sem,
):
    rows, cols = depth_ref.shape
    level_ref, discharge_ref = out_ref.at[0], out_ref.at[1]
    total = depth_ext.shape[1]
    bands = total // SUB
    wide = cols + LANES
    own = cols // LANES
    my_row, my_col = lax.axis_index("row"), lax.axis_index("col")

    def exists(dr, dc):
        r, c = my_row + dr, my_col + dc
        ok = None
        for test in ((r >= 0, r < row_peers) if dr else ()) + ((c >= 0, c < col_peers) if dc else ()):
            ok = test if ok is None else jnp.logical_and(ok, test)
        return ok

    def row_place(dr, width):
        if dr == 0:
            return (pl.ds(0, rows), pl.ds(0, rows))
        if dr < 0:
            return (pl.ds(0, width), pl.ds(rows, width))
        return (pl.ds(rows - width, width), pl.ds(total - width, width))

    def col_place(dc):
        if dc == 0:
            return (pl.ds(0, own), pl.ds(0, own))
        if dc < 0:
            return (pl.ds(0, 1), pl.ds(own, 1))
        return (pl.ds(own - 1, 1), pl.ds(own + 1, 1))

    def copy(slot, k, src, dst, width):
        dr, dc = OFFSETS[k]
        (rs, rd), (cs, cd) = row_place(dr, width), col_place(dc)
        return pltpu.make_async_remote_copy(
            src_ref=src.at[cs, rs],
            dst_ref=dst.at[cd, rd],
            send_sem=send_sem.at[slot, k],
            recv_sem=recv_sem.at[slot, k],
            device_id=(my_row + dr, my_col + dc),
            device_id_type=MESH,
        )

    every = (1, 3, 5, 7, 2, 6, 0, 4)
    slanted = (1, 3, 5, 7, 2, 6)
    straight, corners = (2, 6, 0, 4), (1, 3, 5, 7)

    def send(slot, src, dst, width, order=every):
        for k in order:
            @pl.when(exists(*OFFSETS[k]))
            def _(k=k):
                copy(slot, k, src, dst, width).start()

    def receive(slot, src, dst, width, order=every):
        for k in order:
            dr, dc = OFFSETS[k]
            there = exists(-dr, -dc)

            @pl.when(there)
            def _(k=k):
                copy(slot, k, src, dst, width).wait_recv()

            @pl.when(jnp.logical_not(there))
            def _(dr=dr, dc=dc):
                _, rd = row_place(dr, width)
                _, cd = col_place(dc)
                dst[cd, rd] = jnp.zeros((cd.size, rd.size, LANES), dst.dtype)

    def sent_out(slot, src, dst, width, order=every):
        for k in order:
            @pl.when(exists(*OFFSETS[k]))
            def _(k=k):
                copy(slot, k, src, dst, width).wait_send()

    barrier = pltpu.get_barrier_semaphore()
    for dr, dc in OFFSETS:
        @pl.when(exists(dr, dc))
        def _(dr=dr, dc=dc):
            pl.semaphore_signal(
                barrier, inc=1, device_id=(my_row + dr, my_col + dc), device_id_type=MESH
            )
    staged = (
        (depth_hbm, depth_ref), (rain_hbm, rain_ref), (conv_hbm, conv_ref),
        (dir_hbm, dir_ref), (outlet_hbm, outlet_ref),
    )
    loads = [pltpu.make_async_copy(src, dst, load_sem.at[i]) for i, (src, dst) in enumerate(staged)]
    for load in loads:
        load.start()
    for load in loads:
        load.wait()
    for c in range(own):
        at = pl.ds(c * LANES, LANES)
        mine = pl.ds(0, rows)
        depth_ext[c, mine] = depth_ref[:, at]
        rain_ext[c, mine] = rain_ref[:, at]
        code = dir_ref[:, at]
        route = jnp.where(outlet_ref[:, at] == 1, 0, code + 1)
        route_ext[c, mine] = route
        far_ext[c, mine] = route
        coef_ext[c, mine] = conv_ref[:, at] * jnp.where(
            (code & 1) == 1, jnp.float32(0.70710678), jnp.float32(1.0)
        )
    def reach(index, peers):
        return 1 + jnp.where(index > 0, 1, 0) + jnp.where(index < peers - 1, 1, 0)

    pl.semaphore_wait(barrier, reach(my_row, row_peers) * reach(my_col, col_peers) - 1)

    firsts = (depth_ext, coef_ext, rain_ext, route_ext)
    far_slot, level_slot = (len(firsts), len(firsts) + 1)
    for slot, ext in enumerate(firsts):
        send(slot, ext, ext, NEAR)
    send(far_slot, far_ext, far_ext, MARGIN, slanted)
    unused = pl.ds(rows + NEAR, total - rows - 2 * NEAR)
    for ext in firsts:
        ext[:, unused] = jnp.zeros((own + 2, total - rows - 2 * NEAR, LANES), ext.dtype)
    if SPARE:
        for ext in (far_ext,) + tuple(acc_ext.at[g] for g in range(GROUPS)):
            ext[:, pl.ds(rows + MARGIN, SPARE)] = jnp.zeros((own + 2, SPARE, LANES), ext.dtype)
    for slot, ext in enumerate(firsts):
        receive(slot, ext, ext, NEAR)
    sides = (pl.ds(own, 2), pl.ds(0, rows))
    far_ext[sides] = route_ext[sides]

    right = lax.broadcasted_iota(jnp.int32, (SUB, LANES), 1) < LANES // 2

    def banded(ext, v):
        def part(c):
            return ext[c, pl.ds(v, SUB, stride=bands), :]

        blocks = [part(c) for c in range(own)]
        blocks.append(jnp.where(right, part(own), part(own + 1)))
        return jnp.concatenate(blocks, axis=1)

    for v in range(bands):
        acc[v] = banded(depth_ext, v)
        rain[v] = banded(rain_ext, v)
        coef[v] = banded(coef_ext, v)

    def above(v, get):
        return get(v - 1) if v else pltpu.roll(get(bands - 1), 1, 0)

    def below(v, get):
        return get(v + 1) if v < bands - 1 else pltpu.roll(get(0), SUB - 1, 0)

    def set_masks(ext):
        def routed(v):
            return banded(ext, v)

        for v in range(bands):
            near = {1: above(v, routed), 0: routed(v), -1: below(v, routed)}
            for k, (di, dj) in enumerate(OFFSETS):
                masks[k, v] = jnp.where(near[di] == k + 1, jnp.float32(1.0), jnp.float32(0.0))

    set_masks(route_ext)

    def inflow(v, up, here, down):
        near = {1: up, 0: here, -1: down}
        parts = {}
        for k, (di, dj) in enumerate(OFFSETS):
            term = masks[k, v] * near[di]
            parts[dj] = parts[dj] + term if dj in parts else term
        return parts[0] + (pltpu.roll(parts[1], 1, 1) + pltpu.roll(parts[-1], wide - 1, 1))

    def sweep(field, finish):
        start = field[0]
        up, here = (pltpu.roll(field[bands - 1], 1, 0), start)
        for v in range(bands):
            down = field[v + 1] if v < bands - 1 else pltpu.roll(start, SUB - 1, 0)
            finish(v, inflow(v, up, here, down))
            up, here = here, down

    @pl.loop(0, SUBSTEPS)
    def _(step):
        for v in range(bands):
            h = acc[v]
            factor = coef[v] * jnp.exp(jnp.log(h) * jnp.float32(2.0 / 3.0))
            out = h * (factor / (1.0 + factor))
            share[v] = out
            level[v] = h + rain[v] - out

        def finish(v, came):
            acc[v] = level[v] + came

        sweep(share, finish)

    def finish(v, came):
        acc[v] = level[v] + came

    def passes(count):
        @pl.loop(0, count)
        def _(index):
            sweep(acc, finish)

    def to_plain(field, dst):
        for v in range(bands):
            value = field[v]
            for c in range(own):
                dst[c, pl.ds(v, SUB, stride=bands), :] = value[:, c * LANES : (c + 1) * LANES]

    sub = lax.broadcasted_iota(jnp.int32, (SUB, LANES), 0)

    lane_part = lax.broadcasted_iota(jnp.int32, (SUB, LANES), 1) // MARGIN

    def corner(group, k):
        dr, dc = OFFSETS[k]
        slot = level_slot + group
        return pltpu.make_async_remote_copy(
            src_ref=pack_out.at[group, k],
            dst_ref=pack_in.at[group, k],
            send_sem=send_sem.at[slot, k],
            recv_sem=recv_sem.at[slot, k],
            device_id=(my_row + dr, my_col + dc),
            device_id_type=MESH,
        )

    def send_corners(group, src):
        for k in corners:
            dr, dc = OFFSETS[k]
            start = 0 if dr < 0 else rows - MARGIN
            block, first = (0, 0) if dc < 0 else (own - 1, LANES - MARGIN)
            packed = None
            for g in range(MARGIN // SUB):
                piece = src[block, pl.ds(start + g * SUB, SUB), :]
                shift = (g * MARGIN - first) % LANES
                piece = pltpu.roll(piece, shift, 1) if shift else piece
                packed = piece if packed is None else jnp.where(lane_part == g, piece, packed)
            pack_out[group, k] = packed
        for k in corners:
            @pl.when(exists(*OFFSETS[k]))
            def _(k=k):
                corner(group, k).start()

    def receive_corners(group, dst):
        for k in corners:
            dr, dc = OFFSETS[k]
            there = exists(-dr, -dc)
            start = rows if dr < 0 else total - MARGIN
            block, first = (own, 0) if dc < 0 else (own + 1, LANES - MARGIN)

            @pl.when(there)
            def _(k=k, start=start, block=block, first=first):
                corner(group, k).wait_recv()
                packed = pack_in[group, k]
                for g in range(MARGIN // SUB):
                    shift = (first - g * MARGIN) % LANES
                    piece = pltpu.roll(packed, shift, 1) if shift else packed
                    dst[block, pl.ds(start + g * SUB, SUB), :] = piece

            @pl.when(jnp.logical_not(there))
            def _(start=start, block=block):
                dst[block, pl.ds(start, MARGIN), :] = jnp.zeros((MARGIN, LANES), dst.dtype)

    def widen(src, dst, group, meanwhile, fields):
        slot = level_slot + group
        to_plain(acc, src)
        send_corners(group, src)
        send(slot, src, dst, MARGIN, straight)
        meanwhile()
        receive(slot, src, dst, MARGIN, straight)
        receive_corners(group, dst)
        for v in range(bands):
            inner = sub * bands + v < rows
            for c in range(own):
                at = pl.ds(c * LANES, LANES)
                value = jnp.where(inner, acc[v, :, at], dst[c, pl.ds(v, SUB, stride=bands), :])
                for field in fields:
                    field[v, :, at] = value
            value = jnp.where(
                right,
                dst[own, pl.ds(v, SUB, stride=bands), :],
                dst[own + 1, pl.ds(v, SUB, stride=bands), :],
            )
            for field in fields:
                field[v, :, pl.ds(cols, LANES)] = value

    def in_flight():
        for c in range(own):
            level_ref[:, pl.ds(c * LANES, LANES)] = plain[0, c, pl.ds(0, rows), :]
        receive(far_slot, far_ext, far_ext, MARGIN, slanted)
        set_masks(far_ext)

    widen(plain.at[0], acc_ext.at[0], 0, in_flight, (acc, level))
    passes(MARGIN)
    for group in range(1, GROUPS):
        widen(plain.at[group], acc_ext.at[group], group, lambda: None, (acc,))
        passes(MARGIN)

    to_plain(acc, plain.at[GROUPS])
    for c in range(own):
        discharge_ref[:, pl.ds(c * LANES, LANES)] = jnp.log(1.0 + plain[GROUPS, c, pl.ds(0, rows), :])
    for slot, ext in enumerate(firsts):
        sent_out(slot, ext, ext, NEAR)
    sent_out(far_slot, far_ext, far_ext, MARGIN, slanted)
    for group in range(GROUPS):
        sent_out(level_slot + group, plain.at[group], acc_ext.at[group], MARGIN, straight)
        for k in corners:
            @pl.when(exists(*OFFSETS[k]))
            def _(group=group, k=k):
                corner(group, k).wait_send()


def solution(mesh):
    row_peers, col_peers = mesh.shape["row"], mesh.shape["col"]

    def on_device(depth, rainfall, conveyance, flow_dir, outlet):
        rows, cols = depth.shape
        total = rows + 2 * MARGIN + SPARE
        bands = total // SUB
        wide = cols + LANES
        slots = 5 + GROUPS
        own = cols // LANES
        ext = (own + 2, total, LANES)
        field = (bands, SUB, wide)
        vmem = pl.BlockSpec(memory_space=pltpu.VMEM)
        f32 = jnp.float32
        hbm = pl.BlockSpec(memory_space=pltpu.HBM)
        tile = (rows, cols)
        both = pl.pallas_call(
            functools.partial(kernel, row_peers, col_peers),
            out_shape=jax.ShapeDtypeStruct((2, rows, cols), f32),
            in_specs=[hbm] * 5,
            out_specs=vmem,
            scratch_shapes=[
                pltpu.VMEM(tile, f32),
                pltpu.VMEM(tile, f32),
                pltpu.VMEM(tile, f32),
                pltpu.VMEM(tile, jnp.int32),
                pltpu.VMEM(tile, jnp.int32),
                pltpu.SemaphoreType.DMA((5,)),
                pltpu.VMEM(ext, f32),
                pltpu.VMEM(ext, f32),
                pltpu.VMEM(ext, f32),
                pltpu.VMEM(ext, jnp.int32),
                pltpu.VMEM(ext, jnp.int32),
                pltpu.VMEM((GROUPS,) + ext, f32),
                pltpu.VMEM((GROUPS + 1, own, total, LANES), f32),
                pltpu.VMEM((GROUPS, len(OFFSETS), SUB, LANES), f32),
                pltpu.VMEM((GROUPS, len(OFFSETS), SUB, LANES), f32),
                pltpu.VMEM(field, f32),
                pltpu.VMEM(field, f32),
                pltpu.VMEM(field, f32),
                pltpu.VMEM(field, f32),
                pltpu.VMEM(field, f32),
                pltpu.VMEM((len(OFFSETS),) + field, f32),
                pltpu.SemaphoreType.DMA((slots, len(OFFSETS))),
                pltpu.SemaphoreType.DMA((slots, len(OFFSETS))),
            ],
            compiler_params=pltpu.CompilerParams(
                collective_id=0, has_side_effects=True, vmem_limit_bytes=VMEM_BYTES
            ),
        )(*(
            pltpu.with_memory_space_constraint(a, pltpu.HBM)
            for a in (depth, rainfall, conveyance, flow_dir, outlet)
        ))
        return both[0], both[1]

    placed = P("row", "col")
    return jax.shard_map(
        on_device,
        mesh=mesh,
        in_specs=(placed,) * 5,
        out_specs=(placed, placed),
        check_vma=False,
    )
```

```python
import functools

import jax
import jax.numpy as jnp
from jax import lax
from jax.experimental import pallas as pl
from jax.experimental.pallas import tpu as pltpu
from jax.sharding import PartitionSpec as P

SUBSTEPS = 3
PASSES = 64
OFFSETS = ((0, 1), (1, 1), (1, 0), (1, -1), (0, -1), (-1, -1), (-1, 0), (-1, 1))
LANES = 128
SUB = 8
NEAR = 8
MARGIN = 32
GROUPS = PASSES // MARGIN
SPARE = 0
HALF = LANES // 2
REACH = 3
VMEM_BYTES = 40 * 1024 * 1024
MESH = pl.DeviceIdType.MESH


def kernel(
    row_peers, col_peers,
    depth_hbm, rain_hbm, conv_hbm, dir_hbm, outlet_hbm,
    out_ref,
    depth_ref, rain_ref, conv_ref, dir_ref, outlet_ref, load_sem,
    depth_ext, rain_ext, coef_ext, route_ext, far_ext, acc_ext, plain, pack_out, pack_in,
    acc, rain, coef, level, share, masks,
    send_sem, recv_sem,
):
    rows, cols = depth_ref.shape
    level_ref, discharge_ref = out_ref.at[0], out_ref.at[1]
    total = depth_ext.shape[1]
    bands = total // SUB
    wide = cols + LANES
    own = cols // LANES
    my_row, my_col = lax.axis_index("row"), lax.axis_index("col")

    def exists(dr, dc):
        r, c = my_row + dr, my_col + dc
        ok = None
        for test in ((r >= 0, r < row_peers) if dr else ()) + ((c >= 0, c < col_peers) if dc else ()):
            ok = test if ok is None else jnp.logical_and(ok, test)
        return ok

    def row_place(dr, width):
        if dr == 0:
            return (pl.ds(0, rows), pl.ds(0, rows))
        if dr < 0:
            return (pl.ds(0, width), pl.ds(rows, width))
        return (pl.ds(rows - width, width), pl.ds(total - width, width))

    def col_place(dc):
        if dc == 0:
            return (pl.ds(0, own), pl.ds(0, own))
        if dc < 0:
            return (pl.ds(0, 1), pl.ds(own, 1))
        return (pl.ds(own - 1, 1), pl.ds(own + 1, 1))

    def copy(slot, k, src, dst, width):
        dr, dc = OFFSETS[k]
        (rs, rd), (cs, cd) = row_place(dr, width), col_place(dc)
        return pltpu.make_async_remote_copy(
            src_ref=src.at[cs, rs],
            dst_ref=dst.at[cd, rd],
            send_sem=send_sem.at[slot, k],
            recv_sem=recv_sem.at[slot, k],
            device_id=(my_row + dr, my_col + dc),
            device_id_type=MESH,
        )

    every = (1, 3, 5, 7, 2, 6, 0, 4)
    slanted = (1, 3, 5, 7, 2, 6)
    straight, corners = (2, 6, 0, 4), (1, 3, 5, 7)

    def send(slot, src, dst, width, order=every):
        for k in order:
            @pl.when(exists(*OFFSETS[k]))
            def _(k=k):
                copy(slot, k, src, dst, width).start()

    def receive(slot, src, dst, width, order=every):
        for k in order:
            dr, dc = OFFSETS[k]
            there = exists(-dr, -dc)

            @pl.when(there)
            def _(k=k):
                copy(slot, k, src, dst, width).wait_recv()

            @pl.when(jnp.logical_not(there))
            def _(dr=dr, dc=dc):
                _, rd = row_place(dr, width)
                _, cd = col_place(dc)
                dst[cd, rd] = jnp.zeros((cd.size, rd.size, LANES), dst.dtype)

    def sent_out(slot, src, dst, width, order=every):
        for k in order:
            @pl.when(exists(*OFFSETS[k]))
            def _(k=k):
                copy(slot, k, src, dst, width).wait_send()

    barrier = pltpu.get_barrier_semaphore()
    for dr, dc in OFFSETS:
        @pl.when(exists(dr, dc))
        def _(dr=dr, dc=dc):
            pl.semaphore_signal(
                barrier, inc=1, device_id=(my_row + dr, my_col + dc), device_id_type=MESH
            )
    staged = (
        (depth_hbm, depth_ref), (rain_hbm, rain_ref), (conv_hbm, conv_ref),
        (dir_hbm, dir_ref), (outlet_hbm, outlet_ref),
    )
    loads = [pltpu.make_async_copy(src, dst, load_sem.at[i]) for i, (src, dst) in enumerate(staged)]
    for load in loads:
        load.start()
    for load in loads:
        load.wait()
    for c in range(own):
        at = pl.ds(c * LANES, LANES)
        mine = pl.ds(0, rows)
        depth_ext[c, mine] = depth_ref[:, at]
        rain_ext[c, mine] = rain_ref[:, at]
        code = dir_ref[:, at]
        route = jnp.where(outlet_ref[:, at] == 1, 0, code + 1)
        route_ext[c, mine] = route
        far_ext[c, mine] = route
        coef_ext[c, mine] = conv_ref[:, at] * jnp.where(
            (code & 1) == 1, jnp.float32(0.70710678), jnp.float32(1.0)
        )
    def reach(index, peers):
        return 1 + jnp.where(index > 0, 1, 0) + jnp.where(index < peers - 1, 1, 0)

    pl.semaphore_wait(barrier, reach(my_row, row_peers) * reach(my_col, col_peers) - 1)

    firsts = (depth_ext, coef_ext, rain_ext, route_ext)
    far_slot, level_slot = (len(firsts), len(firsts) + 1)
    for slot, ext in enumerate(firsts):
        send(slot, ext, ext, NEAR)
    send(far_slot, far_ext, far_ext, MARGIN, slanted)
    unused = pl.ds(rows + NEAR, total - rows - 2 * NEAR)
    for ext in firsts:
        ext[:, unused] = jnp.zeros((own + 2, total - rows - 2 * NEAR, LANES), ext.dtype)
    if SPARE:
        for ext in (far_ext,) + tuple(acc_ext.at[g] for g in range(GROUPS)):
            ext[:, pl.ds(rows + MARGIN, SPARE)] = jnp.zeros((own + 2, SPARE, LANES), ext.dtype)
    for slot, ext in enumerate(firsts):
        receive(slot, ext, ext, NEAR)
    sides = (pl.ds(own, 2), pl.ds(0, rows))
    far_ext[sides] = route_ext[sides]

    right = lax.broadcasted_iota(jnp.int32, (SUB, LANES), 1) < LANES // 2

    def banded(ext, v):
        def part(c):
            return ext[c, pl.ds(v, SUB, stride=bands), :]

        blocks = [part(c) for c in range(own)]
        blocks.append(jnp.where(right, part(own), part(own + 1)))
        return jnp.concatenate(blocks, axis=1)

    for v in range(bands):
        acc[v] = banded(depth_ext, v)
        rain[v] = banded(rain_ext, v)
        coef[v] = banded(coef_ext, v)

    def above(v, get):
        return get(v - 1) if v else pltpu.roll(get(bands - 1), 1, 0)

    def below(v, get):
        return get(v + 1) if v < bands - 1 else pltpu.roll(get(0), SUB - 1, 0)

    def set_masks(ext):
        def routed(v):
            return banded(ext, v)

        for v in range(bands):
            near = {1: above(v, routed), 0: routed(v), -1: below(v, routed)}
            for k, (di, dj) in enumerate(OFFSETS):
                masks[k, v] = jnp.where(near[di] == k + 1, jnp.float32(1.0), jnp.float32(0.0))

    set_masks(route_ext)

    def inflow(v, up, here, down):
        near = {1: up, 0: here, -1: down}
        parts = {}
        for k, (di, dj) in enumerate(OFFSETS):
            term = masks[k, v] * near[di]
            parts[dj] = parts[dj] + term if dj in parts else term
        return parts[0] + (pltpu.roll(parts[1], 1, 1) + pltpu.roll(parts[-1], wide - 1, 1))

    def sweep(field, finish):
        start = field[0]
        up, here = (pltpu.roll(field[bands - 1], 1, 0), start)
        for v in range(bands):
            down = field[v + 1] if v < bands - 1 else pltpu.roll(start, SUB - 1, 0)
            finish(v, inflow(v, up, here, down))
            up, here = here, down

    @pl.loop(0, SUBSTEPS)
    def _(step):
        for v in range(bands):
            h = acc[v]
            factor = coef[v] * jnp.exp(jnp.log(h) * jnp.float32(2.0 / 3.0))
            out = h * (factor / (1.0 + factor))
            share[v] = out
            level[v] = h + rain[v] - out

        def finish(v, came):
            acc[v] = level[v] + came

        sweep(share, finish)

    def finish(v, came):
        acc[v] = level[v] + came

    def passes(count):
        @pl.loop(0, count)
        def _(index):
            sweep(acc, finish)

    def to_plain(field, dst):
        for v in range(bands):
            value = field[v]
            for c in range(own):
                dst[c, pl.ds(v, SUB, stride=bands), :] = value[:, c * LANES : (c + 1) * LANES]

    sub = lax.broadcasted_iota(jnp.int32, (SUB, LANES), 0)

    lane_part = lax.broadcasted_iota(jnp.int32, (SUB, LANES), 1) // MARGIN

    def corner(group, k):
        dr, dc = OFFSETS[k]
        slot = level_slot + group
        return pltpu.make_async_remote_copy(
            src_ref=pack_out.at[group, k],
            dst_ref=pack_in.at[group, k],
            send_sem=send_sem.at[slot, k],
            recv_sem=recv_sem.at[slot, k],
            device_id=(my_row + dr, my_col + dc),
            device_id_type=MESH,
        )

    def send_corners(group, src):
        for k in corners:
            dr, dc = OFFSETS[k]
            start = 0 if dr < 0 else rows - MARGIN
            block, first = (0, 0) if dc < 0 else (own - 1, LANES - MARGIN)
            packed = None
            for g in range(MARGIN // SUB):
                piece = src[block, pl.ds(start + g * SUB, SUB), :]
                shift = (g * MARGIN - first) % LANES
                piece = pltpu.roll(piece, shift, 1) if shift else piece
                packed = piece if packed is None else jnp.where(lane_part == g, piece, packed)
            pack_out[group, k] = packed
        for k in corners:
            @pl.when(exists(*OFFSETS[k]))
            def _(k=k):
                corner(group, k).start()

    def receive_corners(group, dst):
        for k in corners:
            dr, dc = OFFSETS[k]
            there = exists(-dr, -dc)
            start = rows if dr < 0 else total - MARGIN
            block, first = (own, 0) if dc < 0 else (own + 1, LANES - MARGIN)

            @pl.when(there)
            def _(k=k, start=start, block=block, first=first):
                corner(group, k).wait_recv()
                packed = pack_in[group, k]
                for g in range(MARGIN // SUB):
                    shift = (first - g * MARGIN) % LANES
                    piece = pltpu.roll(packed, shift, 1) if shift else packed
                    dst[block, pl.ds(start + g * SUB, SUB), :] = piece

            @pl.when(jnp.logical_not(there))
            def _(start=start, block=block):
                dst[block, pl.ds(start, MARGIN), :] = jnp.zeros((MARGIN, LANES), dst.dtype)

    def widen(src, dst, group, meanwhile, fields):
        slot = level_slot + group
        to_plain(acc, src)
        send_corners(group, src)
        send(slot, src, dst, MARGIN, straight)
        meanwhile()
        receive(slot, src, dst, MARGIN, straight)
        receive_corners(group, dst)
        for v in range(bands):
            inner = sub * bands + v < rows
            for c in range(own):
                at = pl.ds(c * LANES, LANES)
                value = jnp.where(inner, acc[v, :, at], dst[c, pl.ds(v, SUB, stride=bands), :])
                for field in fields:
                    field[v, :, at] = value
            value = jnp.where(
                right,
                dst[own, pl.ds(v, SUB, stride=bands), :],
                dst[own + 1, pl.ds(v, SUB, stride=bands), :],
            )
            for field in fields:
                field[v, :, pl.ds(cols, LANES)] = value

    def in_flight():
        for c in range(own):
            level_ref[:, pl.ds(c * LANES, LANES)] = plain[0, c, pl.ds(0, rows), :]
        receive(far_slot, far_ext, far_ext, MARGIN, slanted)
        set_masks(far_ext)

    widen(plain.at[0], acc_ext.at[0], 0, in_flight, (acc, level))
    passes(MARGIN)
    for group in range(1, GROUPS):
        widen(plain.at[group], acc_ext.at[group], group, lambda: None, (acc,))
        passes(MARGIN)

    to_plain(acc, plain.at[GROUPS])
    for c in range(own):
        discharge_ref[:, pl.ds(c * LANES, LANES)] = jnp.log(1.0 + plain[GROUPS, c, pl.ds(0, rows), :])
    for slot, ext in enumerate(firsts):
        sent_out(slot, ext, ext, NEAR)
    sent_out(far_slot, far_ext, far_ext, MARGIN, slanted)
    for group in range(GROUPS):
        sent_out(level_slot + group, plain.at[group], acc_ext.at[group], MARGIN, straight)
        for k in corners:
            @pl.when(exists(*OFFSETS[k]))
            def _(group=group, k=k):
                corner(group, k).wait_send()


def strip_kernel(
    row_peers, col_peers,
    depth_hbm, rain_hbm, conv_hbm, dir_hbm, outlet_hbm,
    out_ref,
    conv_ref, dir_ref, outlet_ref,
    near, rows_out, rows_in, plain,
    h, rain, coef, base, share, near_masks,
    shifted, window,
    acc, level, masks, result,
    load_sem, near_send, near_recv, peer_send, peer_recv,
):
    rows, cols = conv_ref.shape
    own = cols // LANES
    total = plain.shape[1]
    thin = total // SUB
    east, west = own, own + 1
    wide = cols + 2 * LANES
    full = row_peers * rows
    bands = full // SUB
    span = 2 * LANES
    f32 = jnp.float32
    my_row, my_col = lax.axis_index("row"), lax.axis_index("col")

    def exists(dr, dc):
        r, c = my_row + dr, my_col + dc
        return (r >= 0) & (r < row_peers) & (c >= 0) & (c < col_peers)

    barrier = pltpu.get_barrier_semaphore()

    def greet(row, col):
        pl.semaphore_signal(barrier, inc=1, device_id=(row, col), device_id_type=MESH)

    expected = row_peers - 1
    for dr, dc in OFFSETS:
        @pl.when(exists(dr, dc))
        def _(dr=dr, dc=dc):
            greet(my_row + dr, my_col + dc)
        if dc:
            expected = expected + jnp.where(exists(dr, dc), 1, 0)
    for q in range(row_peers):
        far = (my_row - q >= 2) | (q - my_row >= 2)

        @pl.when(far)
        def _(q=q):
            greet(q, my_col)

    loads = [
        pltpu.make_async_copy(src, dst, load_sem.at[i])
        for i, (src, dst) in enumerate(
            [(conv_hbm, conv_ref), (dir_hbm, dir_ref), (outlet_hbm, outlet_ref)]
            + [
                (src.at[:, pl.ds(c * LANES, LANES)], near.at[a, c, pl.ds(0, rows)])
                for a, src in enumerate((depth_hbm, rain_hbm))
                for c in range(own)
            ]
        )
    ]
    for load in loads:
        load.start()
    for load in loads:
        load.wait()

    low = lax.broadcasted_iota(jnp.int32, (SUB, LANES), 1) < HALF

    for c in range(own):
        at = pl.ds(c * LANES, LANES)
        code = dir_ref[:, at]
        near[2, c, pl.ds(0, rows)] = conv_ref[:, at] * jnp.where(
            (code & 1) == 1, f32(0.70710678), f32(1.0)
        )
        near[3, c, pl.ds(0, rows)] = jnp.where(outlet_ref[:, at] == 1, 0, code + 1).astype(f32)

    for a in range(4):
        for c in range(own):
            at = pl.ds((a * own + c) * REACH, REACH)
            rows_out[0, at] = near[a, c, pl.ds(0, REACH)]
            rows_out[1, at] = near[a, c, pl.ds(rows - REACH, REACH)]

    def shift_tiles(field, get, blocks):
        for t in range(rows // SUB):
            tile = pl.ds(t * SUB, SUB)
            turned = {}
            for j in blocks:
                for c in (j - 1, j):
                    if c not in turned:
                        turned[c] = pltpu.roll(get(west if c < 0 else c, tile), HALF, 1)
                shifted[field, j, tile] = jnp.where(low, turned[j - 1], turned[j])

    def route_tile(c, tile):
        return near[3, c, tile]

    shift_tiles(0, route_tile, range(1, own))

    def near_ends(k):
        dr, dc = OFFSETS[k]
        if dc == 0:
            part = pl.ds(0, 4 * own * REACH)
            src, dst = (
                (rows_out.at[0, part], rows_in.at[1, part])
                if dr < 0
                else (rows_out.at[1, part], rows_in.at[0, part])
            )
        else:
            rs, rd = {
                0: (pl.ds(0, rows), pl.ds(0, rows)),
                -1: (pl.ds(0, SUB), pl.ds(rows, SUB)),
                1: (pl.ds(rows - SUB, SUB), pl.ds(total - SUB, SUB)),
            }[dr]
            src = near.at[:, 0 if dc < 0 else own - 1, rs]
            dst = near.at[:, east if dc < 0 else west, rd]
        return src, dst

    def near_copy(k):
        dr, dc = OFFSETS[k]
        src, dst = near_ends(k)
        return pltpu.make_async_remote_copy(
            src_ref=src, dst_ref=dst, send_sem=near_send.at[k], recv_sem=near_recv.at[k],
            device_id=(my_row + dr, my_col + dc), device_id_type=MESH,
        )

    def window_copy(field, half, q):
        peer = lax.rem(my_row + q, row_peers)
        return pltpu.make_async_remote_copy(
            src_ref=shifted.at[field, peer + half],
            dst_ref=window.at[field, half, pl.ds(pl.multiple_of(my_row * rows, rows), rows)],
            send_sem=peer_send.at[field, half, q], recv_sem=peer_recv.at[field, half, q],
            device_id=(peer, my_col), device_id_type=MESH,
        )

    def send_window(field, early, late):
        for q in range(1, row_peers):
            peer = lax.rem(my_row + q, row_peers)
            for half in (0, 1):
                edge = peer == (0, row_peers - 1)[half]
                if early and late:
                    window_copy(field, half, q).start()
                else:
                    @pl.when(edge if late else jnp.logical_not(edge))
                    def _(half=half, q=q):
                        window_copy(field, half, q).start()
        if late:
            window[field, :, pl.ds(pl.multiple_of(my_row * rows, rows), rows)] = shifted[
                field, pl.ds(my_row, 2)
            ]

    def receive_window(field):
        for q in range(1, row_peers):
            for half in (0, 1):
                window_copy(field, half, q).wait_recv()

    def window_sent(field):
        for q in range(1, row_peers):
            for half in (0, 1):
                window_copy(field, half, q).wait_send()

    order = (1, 3, 5, 7, 2, 6, 0, 4)
    pl.semaphore_wait(barrier, expected)
    for k in order:
        @pl.when(exists(*OFFSETS[k]))
        def _(k=k):
            near_copy(k).start()
    send_window(0, True, False)

    blank = pl.ds(rows + REACH, total - rows - 2 * REACH)
    near[:, pl.ds(0, own), blank] = jnp.zeros((4, own, total - rows - 2 * REACH, LANES), f32)

    for k in order:
        dr, dc = OFFSETS[k]
        there = exists(-dr, -dc)

        @pl.when(there)
        def _(k=k):
            near_copy(k).wait_recv()

        @pl.when(jnp.logical_not(there))
        def _(k=k):
            dst = near_ends(k)[1]
            dst[...] = jnp.zeros(dst.shape, f32)

    for a in range(4):
        for c in range(own):
            at = pl.ds((a * own + c) * REACH, REACH)
            near[a, c, pl.ds(rows, REACH)] = rows_in[1, at]
            near[a, c, pl.ds(total - REACH, REACH)] = rows_in[0, at]

    shift_tiles(0, route_tile, (0, own))
    send_window(0, False, True)

    def near_band(a, v):
        take = pl.ds(v, SUB, stride=thin)
        return jnp.concatenate([near[a, c, take, :] for c in range(own + 2)], axis=1)

    for v in range(thin):
        h[v] = near_band(0, v)
        rain[v] = near_band(1, v)
        coef[v] = near_band(2, v)
        base[v] = near_band(3, v)

    def mask_rows(dst, count, up, here, down):
        for v in range(count):
            rows_near = {1: up(v), 0: here(v), -1: down(v)}
            for k, (di, dj) in enumerate(OFFSETS):
                dst[k, v] = jnp.where(rows_near[di] == k + 1, f32(1.0), f32(0.0))

    mask_rows(
        near_masks, thin,
        lambda v: base[v - 1] if v else pltpu.roll(base[thin - 1], 1, 0),
        lambda v: base[v],
        lambda v: base[v + 1] if v < thin - 1 else pltpu.roll(base[0], SUB - 1, 0),
    )

    def sweep(field, mask, count, width, finish):
        start = field[0]
        up, here = pltpu.roll(field[count - 1], 1, 0), start
        for v in range(count):
            down = field[v + 1] if v < count - 1 else pltpu.roll(start, SUB - 1, 0)
            rows_near = {1: up, 0: here, -1: down}
            parts = {}
            for k, (di, dj) in enumerate(OFFSETS):
                term = mask[k, v] * rows_near[di]
                parts[dj] = parts[dj] + term if dj in parts else term
            finish(
                v, parts[0] + (pltpu.roll(parts[1], 1, 1) + pltpu.roll(parts[-1], width - 1, 1))
            )
            up, here = here, down

    @pl.loop(0, SUBSTEPS)
    def _(step):
        for v in range(thin):
            depth = h[v]
            factor = coef[v] * jnp.exp(jnp.log(depth) * f32(2.0 / 3.0))
            out = depth * (factor / (1.0 + factor))
            share[v] = out
            base[v] = depth + rain[v] - out

        def finish(v, came):
            h[v] = base[v] + came

        sweep(share, near_masks, thin, wide, finish)

    for v in range(thin):
        value = h[v]
        for c in range(own + 2):
            plain[c, pl.ds(v, SUB, stride=thin), :] = value[:, c * LANES : (c + 1) * LANES]
    shift_tiles(1, lambda c, tile: plain[c, tile], range(own + 1))
    send_window(1, True, True)
    for c in range(own):
        out_ref[0, :, pl.ds(c * LANES, LANES)] = plain[c, pl.ds(0, rows)]

    def band(field, v):
        take = pl.ds(v, SUB, stride=bands)
        return jnp.concatenate([window[field, 0, take, :], window[field, 1, take, :]], axis=1)

    sub = lax.broadcasted_iota(jnp.int32, (SUB, span), 0)
    receive_window(0)
    for v in range(bands):
        level[v] = band(0, v)
    mask_rows(
        masks, bands,
        lambda v: level[v - 1] if v else jnp.where(
            sub == 0, f32(0.0), pltpu.roll(level[bands - 1], 1, 0)
        ),
        lambda v: level[v],
        lambda v: level[v + 1] if v < bands - 1 else jnp.where(
            sub == SUB - 1, f32(0.0), pltpu.roll(level[0], SUB - 1, 0)
        ),
    )
    receive_window(1)
    for v in range(bands):
        value = band(1, v)
        level[v] = value
        acc[v] = value

    def finish(v, came):
        acc[v] = level[v] + came

    @pl.loop(0, PASSES)
    def _(index):
        sweep(acc, masks, bands, span, finish)

    for v in range(bands):
        value = acc[v]
        core = jnp.where(
            low, pltpu.roll(value[:, :LANES], HALF, 1), pltpu.roll(value[:, LANES:], HALF, 1)
        )
        result[pl.ds(v, SUB, stride=bands), :] = jnp.log(1.0 + core)

    mine = pl.ds(pl.multiple_of(my_row * LANES, LANES), LANES)

    def result_copy(q):
        peer = lax.rem(my_row + q, row_peers)
        return pltpu.make_async_remote_copy(
            src_ref=result.at[pl.ds(pl.multiple_of(peer * rows, rows), rows)],
            dst_ref=out_ref.at[1, :, mine],
            send_sem=peer_send.at[2, 0, q], recv_sem=peer_recv.at[2, 0, q],
            device_id=(peer, my_col), device_id_type=MESH,
        )

    for q in range(1, row_peers):
        result_copy(q).start()
    out_ref[1, :, mine] = result[pl.ds(pl.multiple_of(my_row * rows, rows), rows)]
    for k in order:
        @pl.when(exists(*OFFSETS[k]))
        def _(k=k):
            near_copy(k).wait_send()
    window_sent(0)
    window_sent(1)
    for q in range(1, row_peers):
        result_copy(q).wait_recv()
    for q in range(1, row_peers):
        result_copy(q).wait_send()


def strip_call(row_peers, col_peers, rows, cols):
    own = cols // LANES
    total = rows + 2 * SUB
    thin, bands = total // SUB, row_peers * rows // SUB
    f32, i32 = jnp.float32, jnp.int32
    tile = (rows, cols)
    slim = (thin, SUB, cols + 2 * LANES)
    field = (bands, SUB, 2 * LANES)
    return pl.pallas_call(
        functools.partial(strip_kernel, row_peers, col_peers),
        out_shape=jax.ShapeDtypeStruct((2, rows, cols), f32),
        in_specs=[pl.BlockSpec(memory_space=pltpu.HBM)] * 5,
        out_specs=pl.BlockSpec(memory_space=pltpu.VMEM),
        scratch_shapes=[
            pltpu.VMEM(tile, f32),
            pltpu.VMEM(tile, i32),
            pltpu.VMEM(tile, i32),
            pltpu.VMEM((4, own + 2, total + SUB, LANES), f32),
            pltpu.VMEM((2, 4 * own * REACH + SUB, LANES), f32),
            pltpu.VMEM((2, 4 * own * REACH + SUB, LANES), f32),
            pltpu.VMEM((own + 2, total, LANES), f32),
            pltpu.VMEM(slim, f32),
            pltpu.VMEM(slim, f32),
            pltpu.VMEM(slim, f32),
            pltpu.VMEM(slim, f32),
            pltpu.VMEM(slim, f32),
            pltpu.VMEM((len(OFFSETS),) + slim, f32),
            pltpu.VMEM((2, own + 1, rows, LANES), f32),
            pltpu.VMEM((2, 2, row_peers * rows, LANES), f32),
            pltpu.VMEM(field, f32),
            pltpu.VMEM(field, f32),
            pltpu.VMEM((len(OFFSETS),) + field, f32),
            pltpu.VMEM((row_peers * rows, LANES), f32),
            pltpu.SemaphoreType.DMA((3 + 2 * own,)),
            pltpu.SemaphoreType.DMA((len(OFFSETS),)),
            pltpu.SemaphoreType.DMA((len(OFFSETS),)),
            pltpu.SemaphoreType.DMA((3, 2, row_peers)),
            pltpu.SemaphoreType.DMA((3, 2, row_peers)),
        ],
        compiler_params=pltpu.CompilerParams(
            collective_id=0, has_side_effects=True, vmem_limit_bytes=VMEM_BYTES
        ),
    )


def solution(mesh):
    row_peers, col_peers = mesh.shape["row"], mesh.shape["col"]

    def on_device(depth, rainfall, conveyance, flow_dir, outlet):
        rows, cols = depth.shape
        total = rows + 2 * MARGIN + SPARE
        bands = total // SUB
        wide = cols + LANES
        slots = 5 + GROUPS
        own = cols // LANES
        ext = (own + 2, total, LANES)
        field = (bands, SUB, wide)
        vmem = pl.BlockSpec(memory_space=pltpu.VMEM)
        f32 = jnp.float32
        args = tuple(
            pltpu.with_memory_space_constraint(a, pltpu.HBM)
            for a in (depth, rainfall, conveyance, flow_dir, outlet)
        )
        if cols == row_peers * LANES and row_peers > 1 and rows % (2 * SUB) == 0 and PASSES <= HALF:
            both = strip_call(row_peers, col_peers, rows, cols)(*args)
            return both[0], both[1]
        hbm = pl.BlockSpec(memory_space=pltpu.HBM)
        tile = (rows, cols)
        both = pl.pallas_call(
            functools.partial(kernel, row_peers, col_peers),
            out_shape=jax.ShapeDtypeStruct((2, rows, cols), f32),
            in_specs=[hbm] * 5,
            out_specs=vmem,
            scratch_shapes=[
                pltpu.VMEM(tile, f32),
                pltpu.VMEM(tile, f32),
                pltpu.VMEM(tile, f32),
                pltpu.VMEM(tile, jnp.int32),
                pltpu.VMEM(tile, jnp.int32),
                pltpu.SemaphoreType.DMA((5,)),
                pltpu.VMEM(ext, f32),
                pltpu.VMEM(ext, f32),
                pltpu.VMEM(ext, f32),
                pltpu.VMEM(ext, jnp.int32),
                pltpu.VMEM(ext, jnp.int32),
                pltpu.VMEM((GROUPS,) + ext, f32),
                pltpu.VMEM((GROUPS + 1, own, total, LANES), f32),
                pltpu.VMEM((GROUPS, len(OFFSETS), SUB, LANES), f32),
                pltpu.VMEM((GROUPS, len(OFFSETS), SUB, LANES), f32),
                pltpu.VMEM(field, f32),
                pltpu.VMEM(field, f32),
                pltpu.VMEM(field, f32),
                pltpu.VMEM(field, f32),
                pltpu.VMEM(field, f32),
                pltpu.VMEM((len(OFFSETS),) + field, f32),
                pltpu.SemaphoreType.DMA((slots, len(OFFSETS))),
                pltpu.SemaphoreType.DMA((slots, len(OFFSETS))),
            ],
            compiler_params=pltpu.CompilerParams(
                collective_id=0, has_side_effects=True, vmem_limit_bytes=VMEM_BYTES
            ),
        )(*args)
        return both[0], both[1]

    placed = P("row", "col")
    return jax.shard_map(
        on_device,
        mesh=mesh,
        in_specs=(placed,) * 5,
        out_specs=(placed, placed),
        check_vma=False,
    )
```

```python
import functools

import jax
import jax.numpy as jnp
from jax import lax
from jax.experimental import pallas as pl
from jax.experimental.pallas import tpu as pltpu
from jax.sharding import PartitionSpec as P

SUBSTEPS = 3
PASSES = 64
OFFSETS = ((0, 1), (1, 1), (1, 0), (1, -1), (0, -1), (-1, -1), (-1, 0), (-1, 1))
LANES = 128
SUB = 8
NEAR = 8
MARGIN = 32
GROUPS = PASSES // MARGIN
SPARE = 0
HALF = LANES // 2
REACH = 3
VMEM_BYTES = 40 * 1024 * 1024
MESH = pl.DeviceIdType.MESH


def kernel(
    row_peers, col_peers,
    depth_hbm, rain_hbm, conv_hbm, dir_hbm, outlet_hbm,
    out_ref,
    depth_ref, rain_ref, conv_ref, dir_ref, outlet_ref, load_sem,
    depth_ext, rain_ext, coef_ext, route_ext, far_ext, acc_ext, plain, pack_out, pack_in,
    acc, rain, coef, level, share, masks,
    send_sem, recv_sem,
):
    rows, cols = depth_ref.shape
    level_ref, discharge_ref = out_ref.at[0], out_ref.at[1]
    total = depth_ext.shape[1]
    bands = total // SUB
    wide = cols + LANES
    own = cols // LANES
    my_row, my_col = lax.axis_index("row"), lax.axis_index("col")

    def exists(dr, dc):
        r, c = my_row + dr, my_col + dc
        ok = None
        for test in ((r >= 0, r < row_peers) if dr else ()) + ((c >= 0, c < col_peers) if dc else ()):
            ok = test if ok is None else jnp.logical_and(ok, test)
        return ok

    def row_place(dr, width):
        if dr == 0:
            return (pl.ds(0, rows), pl.ds(0, rows))
        if dr < 0:
            return (pl.ds(0, width), pl.ds(rows, width))
        return (pl.ds(rows - width, width), pl.ds(total - width, width))

    def col_place(dc):
        if dc == 0:
            return (pl.ds(0, own), pl.ds(0, own))
        if dc < 0:
            return (pl.ds(0, 1), pl.ds(own, 1))
        return (pl.ds(own - 1, 1), pl.ds(own + 1, 1))

    def copy(slot, k, src, dst, width):
        dr, dc = OFFSETS[k]
        (rs, rd), (cs, cd) = row_place(dr, width), col_place(dc)
        return pltpu.make_async_remote_copy(
            src_ref=src.at[cs, rs],
            dst_ref=dst.at[cd, rd],
            send_sem=send_sem.at[slot, k],
            recv_sem=recv_sem.at[slot, k],
            device_id=(my_row + dr, my_col + dc),
            device_id_type=MESH,
        )

    every = (1, 3, 5, 7, 2, 6, 0, 4)
    slanted = (1, 3, 5, 7, 2, 6)
    straight, corners = (2, 6, 0, 4), (1, 3, 5, 7)

    def send(slot, src, dst, width, order=every):
        for k in order:
            @pl.when(exists(*OFFSETS[k]))
            def _(k=k):
                copy(slot, k, src, dst, width).start()

    def receive(slot, src, dst, width, order=every):
        for k in order:
            dr, dc = OFFSETS[k]
            there = exists(-dr, -dc)

            @pl.when(there)
            def _(k=k):
                copy(slot, k, src, dst, width).wait_recv()

            @pl.when(jnp.logical_not(there))
            def _(dr=dr, dc=dc):
                _, rd = row_place(dr, width)
                _, cd = col_place(dc)
                dst[cd, rd] = jnp.zeros((cd.size, rd.size, LANES), dst.dtype)

    def sent_out(slot, src, dst, width, order=every):
        for k in order:
            @pl.when(exists(*OFFSETS[k]))
            def _(k=k):
                copy(slot, k, src, dst, width).wait_send()

    barrier = pltpu.get_barrier_semaphore()
    for dr, dc in OFFSETS:
        @pl.when(exists(dr, dc))
        def _(dr=dr, dc=dc):
            pl.semaphore_signal(
                barrier, inc=1, device_id=(my_row + dr, my_col + dc), device_id_type=MESH
            )
    staged = (
        (depth_hbm, depth_ref), (rain_hbm, rain_ref), (conv_hbm, conv_ref),
        (dir_hbm, dir_ref), (outlet_hbm, outlet_ref),
    )
    loads = [pltpu.make_async_copy(src, dst, load_sem.at[i]) for i, (src, dst) in enumerate(staged)]
    for load in loads:
        load.start()
    for load in loads:
        load.wait()
    for c in range(own):
        at = pl.ds(c * LANES, LANES)
        mine = pl.ds(0, rows)
        depth_ext[c, mine] = depth_ref[:, at]
        rain_ext[c, mine] = rain_ref[:, at]
        code = dir_ref[:, at]
        route = jnp.where(outlet_ref[:, at] == 1, 0, code + 1)
        route_ext[c, mine] = route
        far_ext[c, mine] = route
        coef_ext[c, mine] = conv_ref[:, at] * jnp.where(
            (code & 1) == 1, jnp.float32(0.70710678), jnp.float32(1.0)
        )
    def reach(index, peers):
        return 1 + jnp.where(index > 0, 1, 0) + jnp.where(index < peers - 1, 1, 0)

    pl.semaphore_wait(barrier, reach(my_row, row_peers) * reach(my_col, col_peers) - 1)

    firsts = (depth_ext, coef_ext, rain_ext, route_ext)
    far_slot, level_slot = (len(firsts), len(firsts) + 1)
    for slot, ext in enumerate(firsts):
        send(slot, ext, ext, NEAR)
    send(far_slot, far_ext, far_ext, MARGIN, slanted)
    unused = pl.ds(rows + NEAR, total - rows - 2 * NEAR)
    for ext in firsts:
        ext[:, unused] = jnp.zeros((own + 2, total - rows - 2 * NEAR, LANES), ext.dtype)
    if SPARE:
        for ext in (far_ext,) + tuple(acc_ext.at[g] for g in range(GROUPS)):
            ext[:, pl.ds(rows + MARGIN, SPARE)] = jnp.zeros((own + 2, SPARE, LANES), ext.dtype)
    for slot, ext in enumerate(firsts):
        receive(slot, ext, ext, NEAR)
    sides = (pl.ds(own, 2), pl.ds(0, rows))
    far_ext[sides] = route_ext[sides]

    right = lax.broadcasted_iota(jnp.int32, (SUB, LANES), 1) < LANES // 2

    def banded(ext, v):
        def part(c):
            return ext[c, pl.ds(v, SUB, stride=bands), :]

        blocks = [part(c) for c in range(own)]
        blocks.append(jnp.where(right, part(own), part(own + 1)))
        return jnp.concatenate(blocks, axis=1)

    for v in range(bands):
        acc[v] = banded(depth_ext, v)
        rain[v] = banded(rain_ext, v)
        coef[v] = banded(coef_ext, v)

    def above(v, get):
        return get(v - 1) if v else pltpu.roll(get(bands - 1), 1, 0)

    def below(v, get):
        return get(v + 1) if v < bands - 1 else pltpu.roll(get(0), SUB - 1, 0)

    def set_masks(ext):
        def routed(v):
            return banded(ext, v)

        for v in range(bands):
            near = {1: above(v, routed), 0: routed(v), -1: below(v, routed)}
            for k, (di, dj) in enumerate(OFFSETS):
                masks[k, v] = jnp.where(near[di] == k + 1, jnp.float32(1.0), jnp.float32(0.0))

    set_masks(route_ext)

    def inflow(v, up, here, down):
        near = {1: up, 0: here, -1: down}
        parts = {}
        for k, (di, dj) in enumerate(OFFSETS):
            term = masks[k, v] * near[di]
            parts[dj] = parts[dj] + term if dj in parts else term
        return parts[0] + (pltpu.roll(parts[1], 1, 1) + pltpu.roll(parts[-1], wide - 1, 1))

    def sweep(field, finish):
        start = field[0]
        up, here = (pltpu.roll(field[bands - 1], 1, 0), start)
        for v in range(bands):
            down = field[v + 1] if v < bands - 1 else pltpu.roll(start, SUB - 1, 0)
            finish(v, inflow(v, up, here, down))
            up, here = here, down

    @pl.loop(0, SUBSTEPS)
    def _(step):
        for v in range(bands):
            h = acc[v]
            factor = coef[v] * jnp.exp(jnp.log(h) * jnp.float32(2.0 / 3.0))
            out = h * (factor / (1.0 + factor))
            share[v] = out
            level[v] = h + rain[v] - out

        def finish(v, came):
            acc[v] = level[v] + came

        sweep(share, finish)

    def finish(v, came):
        acc[v] = level[v] + came

    def passes(count):
        @pl.loop(0, count)
        def _(index):
            sweep(acc, finish)

    def to_plain(field, dst):
        for v in range(bands):
            value = field[v]
            for c in range(own):
                dst[c, pl.ds(v, SUB, stride=bands), :] = value[:, c * LANES : (c + 1) * LANES]

    sub = lax.broadcasted_iota(jnp.int32, (SUB, LANES), 0)

    lane_part = lax.broadcasted_iota(jnp.int32, (SUB, LANES), 1) // MARGIN

    def corner(group, k):
        dr, dc = OFFSETS[k]
        slot = level_slot + group
        return pltpu.make_async_remote_copy(
            src_ref=pack_out.at[group, k],
            dst_ref=pack_in.at[group, k],
            send_sem=send_sem.at[slot, k],
            recv_sem=recv_sem.at[slot, k],
            device_id=(my_row + dr, my_col + dc),
            device_id_type=MESH,
        )

    def send_corners(group, src):
        for k in corners:
            dr, dc = OFFSETS[k]
            start = 0 if dr < 0 else rows - MARGIN
            block, first = (0, 0) if dc < 0 else (own - 1, LANES - MARGIN)
            packed = None
            for g in range(MARGIN // SUB):
                piece = src[block, pl.ds(start + g * SUB, SUB), :]
                shift = (g * MARGIN - first) % LANES
                piece = pltpu.roll(piece, shift, 1) if shift else piece
                packed = piece if packed is None else jnp.where(lane_part == g, piece, packed)
            pack_out[group, k] = packed
        for k in corners:
            @pl.when(exists(*OFFSETS[k]))
            def _(k=k):
                corner(group, k).start()

    def receive_corners(group, dst):
        for k in corners:
            dr, dc = OFFSETS[k]
            there = exists(-dr, -dc)
            start = rows if dr < 0 else total - MARGIN
            block, first = (own, 0) if dc < 0 else (own + 1, LANES - MARGIN)

            @pl.when(there)
            def _(k=k, start=start, block=block, first=first):
                corner(group, k).wait_recv()
                packed = pack_in[group, k]
                for g in range(MARGIN // SUB):
                    shift = (first - g * MARGIN) % LANES
                    piece = pltpu.roll(packed, shift, 1) if shift else packed
                    dst[block, pl.ds(start + g * SUB, SUB), :] = piece

            @pl.when(jnp.logical_not(there))
            def _(start=start, block=block):
                dst[block, pl.ds(start, MARGIN), :] = jnp.zeros((MARGIN, LANES), dst.dtype)

    def widen(src, dst, group, meanwhile, fields):
        slot = level_slot + group
        to_plain(acc, src)
        send_corners(group, src)
        send(slot, src, dst, MARGIN, straight)
        meanwhile()
        receive(slot, src, dst, MARGIN, straight)
        receive_corners(group, dst)
        for v in range(bands):
            inner = sub * bands + v < rows
            for c in range(own):
                at = pl.ds(c * LANES, LANES)
                value = jnp.where(inner, acc[v, :, at], dst[c, pl.ds(v, SUB, stride=bands), :])
                for field in fields:
                    field[v, :, at] = value
            value = jnp.where(
                right,
                dst[own, pl.ds(v, SUB, stride=bands), :],
                dst[own + 1, pl.ds(v, SUB, stride=bands), :],
            )
            for field in fields:
                field[v, :, pl.ds(cols, LANES)] = value

    def in_flight():
        for c in range(own):
            level_ref[:, pl.ds(c * LANES, LANES)] = plain[0, c, pl.ds(0, rows), :]
        receive(far_slot, far_ext, far_ext, MARGIN, slanted)
        set_masks(far_ext)

    widen(plain.at[0], acc_ext.at[0], 0, in_flight, (acc, level))
    passes(MARGIN)
    for group in range(1, GROUPS):
        widen(plain.at[group], acc_ext.at[group], group, lambda: None, (acc,))
        passes(MARGIN)

    to_plain(acc, plain.at[GROUPS])
    for c in range(own):
        discharge_ref[:, pl.ds(c * LANES, LANES)] = jnp.log(1.0 + plain[GROUPS, c, pl.ds(0, rows), :])
    for slot, ext in enumerate(firsts):
        sent_out(slot, ext, ext, NEAR)
    sent_out(far_slot, far_ext, far_ext, MARGIN, slanted)
    for group in range(GROUPS):
        sent_out(level_slot + group, plain.at[group], acc_ext.at[group], MARGIN, straight)
        for k in corners:
            @pl.when(exists(*OFFSETS[k]))
            def _(group=group, k=k):
                corner(group, k).wait_send()


def strip_kernel(
    row_peers, col_peers,
    depth_hbm, rain_hbm, conv_hbm, dir_hbm, outlet_hbm,
    out_ref,
    conv_ref, dir_ref, outlet_ref,
    near, rows_out, rows_in, plain,
    h, rain, coef, base, share, near_masks,
    shifted, window,
    acc, level, masks, hold, tall, result,
    load_sem, near_send, near_recv, peer_send, peer_recv,
):
    rows, cols = conv_ref.shape
    own = cols // LANES
    total = plain.shape[1]
    thin = total // SUB
    east, west = own, own + 1
    wide = cols + 2 * LANES
    span = 2 * LANES
    bands = span // SUB
    f32 = jnp.float32
    my_row, my_col = lax.axis_index("row"), lax.axis_index("col")

    def exists(dr, dc):
        r, c = my_row + dr, my_col + dc
        return (r >= 0) & (r < row_peers) & (c >= 0) & (c < col_peers)

    barrier = pltpu.get_barrier_semaphore()

    def greet(row, col):
        pl.semaphore_signal(barrier, inc=1, device_id=(row, col), device_id_type=MESH)

    expected = row_peers - 1
    for dr, dc in OFFSETS:
        @pl.when(exists(dr, dc))
        def _(dr=dr, dc=dc):
            greet(my_row + dr, my_col + dc)
        if dc:
            expected = expected + jnp.where(exists(dr, dc), 1, 0)
    for q in range(row_peers):
        far = (my_row - q >= 2) | (q - my_row >= 2)

        @pl.when(far)
        def _(q=q):
            greet(q, my_col)

    loads = [
        pltpu.make_async_copy(src, dst, load_sem.at[i])
        for i, (src, dst) in enumerate(
            [(conv_hbm, conv_ref), (dir_hbm, dir_ref), (outlet_hbm, outlet_ref)]
            + [
                (src.at[:, pl.ds(c * LANES, LANES)], near.at[a, c, pl.ds(0, rows)])
                for a, src in enumerate((depth_hbm, rain_hbm))
                for c in range(own)
            ]
        )
    ]
    for load in loads:
        load.start()
    for load in loads:
        load.wait()

    low = lax.broadcasted_iota(jnp.int32, (SUB, LANES), 1) < HALF

    for c in range(own):
        at = pl.ds(c * LANES, LANES)
        code = dir_ref[:, at]
        near[2, c, pl.ds(0, rows)] = conv_ref[:, at] * jnp.where(
            (code & 1) == 1, f32(0.70710678), f32(1.0)
        )
        near[3, c, pl.ds(0, rows)] = jnp.where(outlet_ref[:, at] == 1, 0, code + 1).astype(f32)

    for a in range(4):
        for c in range(own):
            at = pl.ds((a * own + c) * REACH, REACH)
            rows_out[0, at] = near[a, c, pl.ds(0, REACH)]
            rows_out[1, at] = near[a, c, pl.ds(rows - REACH, REACH)]

    def shift_tiles(field, get, blocks):
        for t in range(rows // SUB):
            tile = pl.ds(t * SUB, SUB)
            turned = {}
            for j in blocks:
                for c in (j - 1, j):
                    if c not in turned:
                        turned[c] = pltpu.roll(get(west if c < 0 else c, tile), HALF, 1)
                shifted[field, j, tile] = jnp.where(low, turned[j - 1], turned[j])

    def route_tile(c, tile):
        return near[3, c, tile]

    shift_tiles(0, route_tile, range(1, own))

    def near_ends(k):
        dr, dc = OFFSETS[k]
        if dc == 0:
            part = pl.ds(0, 4 * own * REACH)
            src, dst = (
                (rows_out.at[0, part], rows_in.at[1, part])
                if dr < 0
                else (rows_out.at[1, part], rows_in.at[0, part])
            )
        else:
            rs, rd = {
                0: (pl.ds(0, rows), pl.ds(0, rows)),
                -1: (pl.ds(0, SUB), pl.ds(rows, SUB)),
                1: (pl.ds(rows - SUB, SUB), pl.ds(total - SUB, SUB)),
            }[dr]
            src = near.at[:, 0 if dc < 0 else own - 1, rs]
            dst = near.at[:, east if dc < 0 else west, rd]
        return src, dst

    def near_copy(k):
        dr, dc = OFFSETS[k]
        src, dst = near_ends(k)
        return pltpu.make_async_remote_copy(
            src_ref=src, dst_ref=dst, send_sem=near_send.at[k], recv_sem=near_recv.at[k],
            device_id=(my_row + dr, my_col + dc), device_id_type=MESH,
        )

    def window_copy(field, half, q):
        peer = lax.rem(my_row + q, row_peers)
        return pltpu.make_async_remote_copy(
            src_ref=shifted.at[field, peer + half],
            dst_ref=window.at[field, half, pl.ds(pl.multiple_of(my_row * rows, rows), rows)],
            send_sem=peer_send.at[field, half, q], recv_sem=peer_recv.at[field, half, q],
            device_id=(peer, my_col), device_id_type=MESH,
        )

    def send_window(field, early, late):
        for q in range(1, row_peers):
            peer = lax.rem(my_row + q, row_peers)
            for half in (0, 1):
                edge = peer == (0, row_peers - 1)[half]
                if early and late:
                    window_copy(field, half, q).start()
                else:
                    @pl.when(edge if late else jnp.logical_not(edge))
                    def _(half=half, q=q):
                        window_copy(field, half, q).start()
        if late:
            window[field, :, pl.ds(pl.multiple_of(my_row * rows, rows), rows)] = shifted[
                field, pl.ds(my_row, 2)
            ]

    def receive_window(field):
        for q in range(1, row_peers):
            for half in (0, 1):
                window_copy(field, half, q).wait_recv()

    def window_sent(field):
        for q in range(1, row_peers):
            for half in (0, 1):
                window_copy(field, half, q).wait_send()

    order = (1, 3, 5, 7, 2, 6, 0, 4)
    pl.semaphore_wait(barrier, expected)
    for k in order:
        @pl.when(exists(*OFFSETS[k]))
        def _(k=k):
            near_copy(k).start()
    send_window(0, True, False)

    blank = pl.ds(rows + REACH, total - rows - 2 * REACH)
    near[:, pl.ds(0, own), blank] = jnp.zeros((4, own, total - rows - 2 * REACH, LANES), f32)

    for k in order:
        dr, dc = OFFSETS[k]
        there = exists(-dr, -dc)

        @pl.when(there)
        def _(k=k):
            near_copy(k).wait_recv()

        @pl.when(jnp.logical_not(there))
        def _(k=k):
            dst = near_ends(k)[1]
            dst[...] = jnp.zeros(dst.shape, f32)

    for a in range(4):
        for c in range(own):
            at = pl.ds((a * own + c) * REACH, REACH)
            near[a, c, pl.ds(rows, REACH)] = rows_in[1, at]
            near[a, c, pl.ds(total - REACH, REACH)] = rows_in[0, at]

    shift_tiles(0, route_tile, (0, own))
    send_window(0, False, True)

    def near_band(a, v):
        take = pl.ds(v, SUB, stride=thin)
        return jnp.concatenate([near[a, c, take, :] for c in range(own + 2)], axis=1)

    for v in range(thin):
        h[v] = near_band(0, v)
        rain[v] = near_band(1, v)
        coef[v] = near_band(2, v)
        base[v] = near_band(3, v)

    def mask_rows(dst, count, up, here, down):
        for v in range(count):
            rows_near = {1: up(v), 0: here(v), -1: down(v)}
            for k, (di, dj) in enumerate(OFFSETS):
                dst[k, v] = jnp.where(rows_near[di] == k + 1, f32(1.0), f32(0.0))

    mask_rows(
        near_masks, thin,
        lambda v: base[v - 1] if v else pltpu.roll(base[thin - 1], 1, 0),
        lambda v: base[v],
        lambda v: base[v + 1] if v < thin - 1 else pltpu.roll(base[0], SUB - 1, 0),
    )

    def sweep(field, mask, count, width, finish):
        start = field[0]
        up, here = pltpu.roll(field[count - 1], 1, 0), start
        for v in range(count):
            down = field[v + 1] if v < count - 1 else pltpu.roll(start, SUB - 1, 0)
            rows_near = {1: up, 0: here, -1: down}
            parts = {}
            for k, (di, dj) in enumerate(OFFSETS):
                term = mask[k, v] * rows_near[di]
                parts[dj] = parts[dj] + term if dj in parts else term
            finish(
                v, parts[0] + (pltpu.roll(parts[1], 1, 1) + pltpu.roll(parts[-1], width - 1, 1))
            )
            up, here = here, down

    @pl.loop(0, SUBSTEPS)
    def _(step):
        for v in range(thin):
            depth = h[v]
            factor = coef[v] * jnp.exp(jnp.log(depth) * f32(2.0 / 3.0))
            out = depth * (factor / (1.0 + factor))
            share[v] = out
            base[v] = depth + rain[v] - out

        def finish(v, came):
            h[v] = base[v] + came

        sweep(share, near_masks, thin, wide, finish)

    for v in range(thin):
        value = h[v]
        for c in range(own + 2):
            plain[c, pl.ds(v, SUB, stride=thin), :] = value[:, c * LANES : (c + 1) * LANES]
    shift_tiles(1, lambda c, tile: plain[c, tile], range(own + 1))
    send_window(1, True, True)
    for c in range(own):
        out_ref[0, :, pl.ds(c * LANES, LANES)] = plain[c, pl.ds(0, rows)]

    def lay(field):
        for b in (0, 1):
            for half in (0, 1):
                tall[b, pl.ds(half * LANES, LANES), :] = window[
                    field, half, pl.ds(b, LANES, stride=2), :
                ].T

    def band(v, b):
        return tall[b, pl.ds(v, SUB, stride=bands), :]

    along = lax.broadcasted_iota(jnp.int32, (SUB, LANES), 1)
    receive_window(0)
    lay(0)
    for b in (0, 1):
        for v in range(bands):
            cols_near = {
                1: band(v - 1, b) if v else pltpu.roll(band(bands - 1, b), 1, 0),
                0: band(v, b),
                -1: band(v + 1, b) if v < bands - 1 else pltpu.roll(band(0, b), SUB - 1, 0),
            }
            for k, (di, dj) in enumerate(OFFSETS):
                here = cols_near[dj] == k + 1
                if (di, b) == (1, 1):
                    here = here & (along < LANES - 1)
                elif (di, b) == (-1, 0):
                    here = here & (along > 0)
                masks[k, v, b] = jnp.where(here, f32(1.0), f32(0.0))
    receive_window(1)
    lay(1)
    for v in range(bands):
        for b in (0, 1):
            value = band(v, b)
            level[v, b] = value
            acc[v, b] = value

    def pair(ref, v):
        return ref[v, 0], ref[v, 1]

    def turn(values, amount):
        return tuple(pltpu.roll(value, amount, 0) for value in values)

    def gather(held, seed, left, here, right):
        cols_near = {1: left, 0: here, -1: right}
        parts = {}
        for k, (di, dj) in enumerate(OFFSETS):
            for b in (0, 1):
                term = held[k, b] * cols_near[dj][b]
                parts[di, b] = parts[di, b] + term if (di, b) in parts else term
        return (
            seed[0] + (parts[0, 0] + (parts[-1, 1] + pltpu.roll(parts[1, 1], 1, 1))),
            seed[1] + (parts[0, 1] + (parts[1, 0] + pltpu.roll(parts[-1, 0], LANES - 1, 1))),
        )

    def fetch(v):
        return {(k, b): masks[k, v, b] for k in range(len(OFFSETS)) for b in (0, 1)}

    def put(ref, v, values):
        ref[v, 0], ref[v, 1] = values

    @pl.loop(0, PASSES // 2)
    def _(index):
        left, here = turn(pair(acc, bands - 1), 1), pair(acc, 0)
        older = newer = held = seed = None
        for v in range(bands):
            right = pair(acc, v + 1) if v < bands - 1 else turn(pair(acc, 0), SUB - 1)
            fresh, start = fetch(v), pair(level, v)
            value = gather(fresh, start, left, here, right)
            if v < 2:
                put(hold, v, value)
            else:
                put(acc, v - 1, gather(held, seed, older, newer, value))
            older, newer = newer, value
            held, seed = fresh, start
            left, here = here, right
        put(acc, bands - 1, gather(held, seed, older, newer, turn(pair(hold, 0), SUB - 1)))
        put(
            acc, 0,
            gather(fetch(0), pair(level, 0), turn(newer, 1), pair(hold, 0), pair(hold, 1)),
        )

    for v in range(bands):
        for b in (0, 1):
            tall[b, pl.ds(v, SUB, stride=bands), :] = acc[v, b]
    for b in (0, 1):
        core = jnp.log(1.0 + tall[b, pl.ds(HALF, LANES), :])
        result[pl.ds(b, LANES, stride=2), :] = core.T

    mine = pl.ds(pl.multiple_of(my_row * LANES, LANES), LANES)

    def result_copy(q):
        peer = lax.rem(my_row + q, row_peers)
        return pltpu.make_async_remote_copy(
            src_ref=result.at[pl.ds(pl.multiple_of(peer * rows, rows), rows)],
            dst_ref=out_ref.at[1, :, mine],
            send_sem=peer_send.at[2, 0, q], recv_sem=peer_recv.at[2, 0, q],
            device_id=(peer, my_col), device_id_type=MESH,
        )

    for q in range(1, row_peers):
        result_copy(q).start()
    out_ref[1, :, mine] = result[pl.ds(pl.multiple_of(my_row * rows, rows), rows)]
    for k in order:
        @pl.when(exists(*OFFSETS[k]))
        def _(k=k):
            near_copy(k).wait_send()
    window_sent(0)
    window_sent(1)
    for q in range(1, row_peers):
        result_copy(q).wait_recv()
    for q in range(1, row_peers):
        result_copy(q).wait_send()


def strip_call(row_peers, col_peers, rows, cols):
    own = cols // LANES
    total = rows + 2 * SUB
    thin, bands = total // SUB, 2 * LANES // SUB
    f32, i32 = jnp.float32, jnp.int32
    tile = (rows, cols)
    slim = (thin, SUB, cols + 2 * LANES)
    field = (bands, 2, SUB, LANES)
    return pl.pallas_call(
        functools.partial(strip_kernel, row_peers, col_peers),
        out_shape=jax.ShapeDtypeStruct((2, rows, cols), f32),
        in_specs=[pl.BlockSpec(memory_space=pltpu.HBM)] * 5,
        out_specs=pl.BlockSpec(memory_space=pltpu.VMEM),
        scratch_shapes=[
            pltpu.VMEM(tile, f32),
            pltpu.VMEM(tile, i32),
            pltpu.VMEM(tile, i32),
            pltpu.VMEM((4, own + 2, total + SUB, LANES), f32),
            pltpu.VMEM((2, 4 * own * REACH + SUB, LANES), f32),
            pltpu.VMEM((2, 4 * own * REACH + SUB, LANES), f32),
            pltpu.VMEM((own + 2, total, LANES), f32),
            pltpu.VMEM(slim, f32),
            pltpu.VMEM(slim, f32),
            pltpu.VMEM(slim, f32),
            pltpu.VMEM(slim, f32),
            pltpu.VMEM(slim, f32),
            pltpu.VMEM((len(OFFSETS),) + slim, f32),
            pltpu.VMEM((2, own + 1, rows, LANES), f32),
            pltpu.VMEM((2, 2, row_peers * rows, LANES), f32),
            pltpu.VMEM(field, f32),
            pltpu.VMEM(field, f32),
            pltpu.VMEM((len(OFFSETS),) + field, f32),
            pltpu.VMEM((2, 2, SUB, LANES), f32),
            pltpu.VMEM((2, 2 * LANES, LANES), f32),
            pltpu.VMEM((row_peers * rows, LANES), f32),
            pltpu.SemaphoreType.DMA((3 + 2 * own,)),
            pltpu.SemaphoreType.DMA((len(OFFSETS),)),
            pltpu.SemaphoreType.DMA((len(OFFSETS),)),
            pltpu.SemaphoreType.DMA((3, 2, row_peers)),
            pltpu.SemaphoreType.DMA((3, 2, row_peers)),
        ],
        compiler_params=pltpu.CompilerParams(
            collective_id=0, has_side_effects=True, vmem_limit_bytes=VMEM_BYTES
        ),
    )


def solution(mesh):
    row_peers, col_peers = mesh.shape["row"], mesh.shape["col"]

    def on_device(depth, rainfall, conveyance, flow_dir, outlet):
        rows, cols = depth.shape
        total = rows + 2 * MARGIN + SPARE
        bands = total // SUB
        wide = cols + LANES
        slots = 5 + GROUPS
        own = cols // LANES
        ext = (own + 2, total, LANES)
        field = (bands, SUB, wide)
        vmem = pl.BlockSpec(memory_space=pltpu.VMEM)
        f32 = jnp.float32
        args = tuple(
            pltpu.with_memory_space_constraint(a, pltpu.HBM)
            for a in (depth, rainfall, conveyance, flow_dir, outlet)
        )
        strips = row_peers > 1 and cols == row_peers * LANES and row_peers * rows == 2 * LANES
        if strips and rows % SUB == 0 and PASSES <= HALF and PASSES % 2 == 0:
            both = strip_call(row_peers, col_peers, rows, cols)(*args)
            return both[0], both[1]
        hbm = pl.BlockSpec(memory_space=pltpu.HBM)
        tile = (rows, cols)
        both = pl.pallas_call(
            functools.partial(kernel, row_peers, col_peers),
            out_shape=jax.ShapeDtypeStruct((2, rows, cols), f32),
            in_specs=[hbm] * 5,
            out_specs=vmem,
            scratch_shapes=[
                pltpu.VMEM(tile, f32),
                pltpu.VMEM(tile, f32),
                pltpu.VMEM(tile, f32),
                pltpu.VMEM(tile, jnp.int32),
                pltpu.VMEM(tile, jnp.int32),
                pltpu.SemaphoreType.DMA((5,)),
                pltpu.VMEM(ext, f32),
                pltpu.VMEM(ext, f32),
                pltpu.VMEM(ext, f32),
                pltpu.VMEM(ext, jnp.int32),
                pltpu.VMEM(ext, jnp.int32),
                pltpu.VMEM((GROUPS,) + ext, f32),
                pltpu.VMEM((GROUPS + 1, own, total, LANES), f32),
                pltpu.VMEM((GROUPS, len(OFFSETS), SUB, LANES), f32),
                pltpu.VMEM((GROUPS, len(OFFSETS), SUB, LANES), f32),
                pltpu.VMEM(field, f32),
                pltpu.VMEM(field, f32),
                pltpu.VMEM(field, f32),
                pltpu.VMEM(field, f32),
                pltpu.VMEM(field, f32),
                pltpu.VMEM((len(OFFSETS),) + field, f32),
                pltpu.SemaphoreType.DMA((slots, len(OFFSETS))),
                pltpu.SemaphoreType.DMA((slots, len(OFFSETS))),
            ],
            compiler_params=pltpu.CompilerParams(
                collective_id=0, has_side_effects=True, vmem_limit_bytes=VMEM_BYTES
            ),
        )(*args)
        return both[0], both[1]

    placed = P("row", "col")
    return jax.shard_map(
        on_device,
        mesh=mesh,
        in_specs=(placed,) * 5,
        out_specs=(placed, placed),
        check_vma=False,
    )
```

```python
import functools

import jax
import jax.numpy as jnp
from jax import lax
from jax.experimental import pallas as pl
from jax.experimental.pallas import tpu as pltpu
from jax.sharding import PartitionSpec as P

SUBSTEPS = 3
PASSES = 64
OFFSETS = ((0, 1), (1, 1), (1, 0), (1, -1), (0, -1), (-1, -1), (-1, 0), (-1, 1))
LANES = 128
SUB = 8
NEAR = 8
MARGIN = 32
GROUPS = PASSES // MARGIN
SPARE = 0
HALF = LANES // 2
REACH = 3
PACK = 2 * SUB
STAGES = (24, 20, 20)
VMEM_BYTES = 40 * 1024 * 1024
MESH = pl.DeviceIdType.MESH


def kernel(
    row_peers, col_peers,
    depth_hbm, rain_hbm, conv_hbm, dir_hbm, outlet_hbm,
    out_ref,
    depth_ref, rain_ref, conv_ref, dir_ref, outlet_ref, load_sem,
    depth_ext, rain_ext, coef_ext, route_ext, far_ext, acc_ext, plain, pack_out, pack_in,
    acc, rain, coef, level, share, masks,
    send_sem, recv_sem,
):
    rows, cols = depth_ref.shape
    level_ref, discharge_ref = out_ref.at[0], out_ref.at[1]
    total = depth_ext.shape[1]
    bands = total // SUB
    wide = cols + LANES
    own = cols // LANES
    my_row, my_col = lax.axis_index("row"), lax.axis_index("col")

    def exists(dr, dc):
        r, c = my_row + dr, my_col + dc
        ok = None
        for test in ((r >= 0, r < row_peers) if dr else ()) + ((c >= 0, c < col_peers) if dc else ()):
            ok = test if ok is None else jnp.logical_and(ok, test)
        return ok

    def row_place(dr, width):
        if dr == 0:
            return (pl.ds(0, rows), pl.ds(0, rows))
        if dr < 0:
            return (pl.ds(0, width), pl.ds(rows, width))
        return (pl.ds(rows - width, width), pl.ds(total - width, width))

    def col_place(dc):
        if dc == 0:
            return (pl.ds(0, own), pl.ds(0, own))
        if dc < 0:
            return (pl.ds(0, 1), pl.ds(own, 1))
        return (pl.ds(own - 1, 1), pl.ds(own + 1, 1))

    def copy(slot, k, src, dst, width):
        dr, dc = OFFSETS[k]
        (rs, rd), (cs, cd) = row_place(dr, width), col_place(dc)
        return pltpu.make_async_remote_copy(
            src_ref=src.at[cs, rs],
            dst_ref=dst.at[cd, rd],
            send_sem=send_sem.at[slot, k],
            recv_sem=recv_sem.at[slot, k],
            device_id=(my_row + dr, my_col + dc),
            device_id_type=MESH,
        )

    every = (1, 3, 5, 7, 2, 6, 0, 4)
    slanted = (1, 3, 5, 7, 2, 6)
    straight, corners = (2, 6, 0, 4), (1, 3, 5, 7)

    def send(slot, src, dst, width, order=every):
        for k in order:
            @pl.when(exists(*OFFSETS[k]))
            def _(k=k):
                copy(slot, k, src, dst, width).start()

    def receive(slot, src, dst, width, order=every):
        for k in order:
            dr, dc = OFFSETS[k]
            there = exists(-dr, -dc)

            @pl.when(there)
            def _(k=k):
                copy(slot, k, src, dst, width).wait_recv()

            @pl.when(jnp.logical_not(there))
            def _(dr=dr, dc=dc):
                _, rd = row_place(dr, width)
                _, cd = col_place(dc)
                dst[cd, rd] = jnp.zeros((cd.size, rd.size, LANES), dst.dtype)

    def sent_out(slot, src, dst, width, order=every):
        for k in order:
            @pl.when(exists(*OFFSETS[k]))
            def _(k=k):
                copy(slot, k, src, dst, width).wait_send()

    barrier = pltpu.get_barrier_semaphore()
    for dr, dc in OFFSETS:
        @pl.when(exists(dr, dc))
        def _(dr=dr, dc=dc):
            pl.semaphore_signal(
                barrier, inc=1, device_id=(my_row + dr, my_col + dc), device_id_type=MESH
            )
    staged = (
        (depth_hbm, depth_ref), (rain_hbm, rain_ref), (conv_hbm, conv_ref),
        (dir_hbm, dir_ref), (outlet_hbm, outlet_ref),
    )
    loads = [pltpu.make_async_copy(src, dst, load_sem.at[i]) for i, (src, dst) in enumerate(staged)]
    for load in loads:
        load.start()
    for load in loads:
        load.wait()
    for c in range(own):
        at = pl.ds(c * LANES, LANES)
        mine = pl.ds(0, rows)
        depth_ext[c, mine] = depth_ref[:, at]
        rain_ext[c, mine] = rain_ref[:, at]
        code = dir_ref[:, at]
        route = jnp.where(outlet_ref[:, at] == 1, 0, code + 1)
        route_ext[c, mine] = route
        far_ext[c, mine] = route
        coef_ext[c, mine] = conv_ref[:, at] * jnp.where(
            (code & 1) == 1, jnp.float32(0.70710678), jnp.float32(1.0)
        )
    def reach(index, peers):
        return 1 + jnp.where(index > 0, 1, 0) + jnp.where(index < peers - 1, 1, 0)

    pl.semaphore_wait(barrier, reach(my_row, row_peers) * reach(my_col, col_peers) - 1)

    firsts = (depth_ext, coef_ext, rain_ext, route_ext)
    far_slot, level_slot = (len(firsts), len(firsts) + 1)
    for slot, ext in enumerate(firsts):
        send(slot, ext, ext, NEAR)
    send(far_slot, far_ext, far_ext, MARGIN, slanted)
    unused = pl.ds(rows + NEAR, total - rows - 2 * NEAR)
    for ext in firsts:
        ext[:, unused] = jnp.zeros((own + 2, total - rows - 2 * NEAR, LANES), ext.dtype)
    if SPARE:
        for ext in (far_ext,) + tuple(acc_ext.at[g] for g in range(GROUPS)):
            ext[:, pl.ds(rows + MARGIN, SPARE)] = jnp.zeros((own + 2, SPARE, LANES), ext.dtype)
    for slot, ext in enumerate(firsts):
        receive(slot, ext, ext, NEAR)
    sides = (pl.ds(own, 2), pl.ds(0, rows))
    far_ext[sides] = route_ext[sides]

    right = lax.broadcasted_iota(jnp.int32, (SUB, LANES), 1) < LANES // 2

    def banded(ext, v):
        def part(c):
            return ext[c, pl.ds(v, SUB, stride=bands), :]

        blocks = [part(c) for c in range(own)]
        blocks.append(jnp.where(right, part(own), part(own + 1)))
        return jnp.concatenate(blocks, axis=1)

    for v in range(bands):
        acc[v] = banded(depth_ext, v)
        rain[v] = banded(rain_ext, v)
        coef[v] = banded(coef_ext, v)

    def above(v, get):
        return get(v - 1) if v else pltpu.roll(get(bands - 1), 1, 0)

    def below(v, get):
        return get(v + 1) if v < bands - 1 else pltpu.roll(get(0), SUB - 1, 0)

    def set_masks(ext):
        def routed(v):
            return banded(ext, v)

        for v in range(bands):
            near = {1: above(v, routed), 0: routed(v), -1: below(v, routed)}
            for k, (di, dj) in enumerate(OFFSETS):
                masks[k, v] = jnp.where(near[di] == k + 1, jnp.float32(1.0), jnp.float32(0.0))

    set_masks(route_ext)

    def inflow(v, up, here, down):
        near = {1: up, 0: here, -1: down}
        parts = {}
        for k, (di, dj) in enumerate(OFFSETS):
            term = masks[k, v] * near[di]
            parts[dj] = parts[dj] + term if dj in parts else term
        return parts[0] + (pltpu.roll(parts[1], 1, 1) + pltpu.roll(parts[-1], wide - 1, 1))

    def sweep(field, finish):
        start = field[0]
        up, here = (pltpu.roll(field[bands - 1], 1, 0), start)
        for v in range(bands):
            down = field[v + 1] if v < bands - 1 else pltpu.roll(start, SUB - 1, 0)
            finish(v, inflow(v, up, here, down))
            up, here = here, down

    @pl.loop(0, SUBSTEPS)
    def _(step):
        for v in range(bands):
            h = acc[v]
            factor = coef[v] * jnp.exp(jnp.log(h) * jnp.float32(2.0 / 3.0))
            out = h * (factor / (1.0 + factor))
            share[v] = out
            level[v] = h + rain[v] - out

        def finish(v, came):
            acc[v] = level[v] + came

        sweep(share, finish)

    def finish(v, came):
        acc[v] = level[v] + came

    def passes(count):
        @pl.loop(0, count)
        def _(index):
            sweep(acc, finish)

    def to_plain(field, dst):
        for v in range(bands):
            value = field[v]
            for c in range(own):
                dst[c, pl.ds(v, SUB, stride=bands), :] = value[:, c * LANES : (c + 1) * LANES]

    sub = lax.broadcasted_iota(jnp.int32, (SUB, LANES), 0)

    lane_part = lax.broadcasted_iota(jnp.int32, (SUB, LANES), 1) // MARGIN

    def corner(group, k):
        dr, dc = OFFSETS[k]
        slot = level_slot + group
        return pltpu.make_async_remote_copy(
            src_ref=pack_out.at[group, k],
            dst_ref=pack_in.at[group, k],
            send_sem=send_sem.at[slot, k],
            recv_sem=recv_sem.at[slot, k],
            device_id=(my_row + dr, my_col + dc),
            device_id_type=MESH,
        )

    def send_corners(group, src):
        for k in corners:
            dr, dc = OFFSETS[k]
            start = 0 if dr < 0 else rows - MARGIN
            block, first = (0, 0) if dc < 0 else (own - 1, LANES - MARGIN)
            packed = None
            for g in range(MARGIN // SUB):
                piece = src[block, pl.ds(start + g * SUB, SUB), :]
                shift = (g * MARGIN - first) % LANES
                piece = pltpu.roll(piece, shift, 1) if shift else piece
                packed = piece if packed is None else jnp.where(lane_part == g, piece, packed)
            pack_out[group, k] = packed
        for k in corners:
            @pl.when(exists(*OFFSETS[k]))
            def _(k=k):
                corner(group, k).start()

    def receive_corners(group, dst):
        for k in corners:
            dr, dc = OFFSETS[k]
            there = exists(-dr, -dc)
            start = rows if dr < 0 else total - MARGIN
            block, first = (own, 0) if dc < 0 else (own + 1, LANES - MARGIN)

            @pl.when(there)
            def _(k=k, start=start, block=block, first=first):
                corner(group, k).wait_recv()
                packed = pack_in[group, k]
                for g in range(MARGIN // SUB):
                    shift = (first - g * MARGIN) % LANES
                    piece = pltpu.roll(packed, shift, 1) if shift else packed
                    dst[block, pl.ds(start + g * SUB, SUB), :] = piece

            @pl.when(jnp.logical_not(there))
            def _(start=start, block=block):
                dst[block, pl.ds(start, MARGIN), :] = jnp.zeros((MARGIN, LANES), dst.dtype)

    def widen(src, dst, group, meanwhile, fields):
        slot = level_slot + group
        to_plain(acc, src)
        send_corners(group, src)
        send(slot, src, dst, MARGIN, straight)
        meanwhile()
        receive(slot, src, dst, MARGIN, straight)
        receive_corners(group, dst)
        for v in range(bands):
            inner = sub * bands + v < rows
            for c in range(own):
                at = pl.ds(c * LANES, LANES)
                value = jnp.where(inner, acc[v, :, at], dst[c, pl.ds(v, SUB, stride=bands), :])
                for field in fields:
                    field[v, :, at] = value
            value = jnp.where(
                right,
                dst[own, pl.ds(v, SUB, stride=bands), :],
                dst[own + 1, pl.ds(v, SUB, stride=bands), :],
            )
            for field in fields:
                field[v, :, pl.ds(cols, LANES)] = value

    def in_flight():
        for c in range(own):
            level_ref[:, pl.ds(c * LANES, LANES)] = plain[0, c, pl.ds(0, rows), :]
        receive(far_slot, far_ext, far_ext, MARGIN, slanted)
        set_masks(far_ext)

    widen(plain.at[0], acc_ext.at[0], 0, in_flight, (acc, level))
    passes(MARGIN)
    for group in range(1, GROUPS):
        widen(plain.at[group], acc_ext.at[group], group, lambda: None, (acc,))
        passes(MARGIN)

    to_plain(acc, plain.at[GROUPS])
    for c in range(own):
        discharge_ref[:, pl.ds(c * LANES, LANES)] = jnp.log(1.0 + plain[GROUPS, c, pl.ds(0, rows), :])
    for slot, ext in enumerate(firsts):
        sent_out(slot, ext, ext, NEAR)
    sent_out(far_slot, far_ext, far_ext, MARGIN, slanted)
    for group in range(GROUPS):
        sent_out(level_slot + group, plain.at[group], acc_ext.at[group], MARGIN, straight)
        for k in corners:
            @pl.when(exists(*OFFSETS[k]))
            def _(group=group, k=k):
                corner(group, k).wait_send()


def stage_plan():
    left, plan = PASSES, []
    for count in STAGES:
        plan.append((count, HALF - left, (LANES + 2 * left) // SUB))
        left -= count
    return plan


def strip_kernel(
    row_peers, col_peers,
    depth_hbm, rain_hbm, conv_hbm, dir_hbm, outlet_hbm,
    out_ref,
    conv_ref, dir_ref, outlet_ref,
    near, rows_out, rows_in, corners_in, plain,
    h, rain, coef, base, share, near_masks,
    shifted, window,
    acc, level, hold, tall, moved, result,
    load_sem, near_send, near_recv, peer_send, peer_recv,
    *stage_masks,
):
    rows, cols = conv_ref.shape
    own = cols // LANES
    total = plain.shape[1]
    thin = total // SUB
    east, west = own, own + 1
    wide = cols + 2 * LANES
    f32 = jnp.float32
    my_row, my_col = lax.axis_index("row"), lax.axis_index("col")

    def exists(dr, dc):
        r, c = my_row + dr, my_col + dc
        return (r >= 0) & (r < row_peers) & (c >= 0) & (c < col_peers)

    barrier = pltpu.get_barrier_semaphore()

    def greet(row, col):
        pl.semaphore_signal(barrier, inc=1, device_id=(row, col), device_id_type=MESH)

    expected = row_peers - 1
    for dr, dc in OFFSETS:
        @pl.when(exists(dr, dc))
        def _(dr=dr, dc=dc):
            greet(my_row + dr, my_col + dc)
        if dc:
            expected = expected + jnp.where(exists(dr, dc), 1, 0)
    for q in range(row_peers):
        far = (my_row - q >= 2) | (q - my_row >= 2)

        @pl.when(far)
        def _(q=q):
            greet(q, my_col)

    loads = [
        pltpu.make_async_copy(src, dst, load_sem.at[i])
        for i, (src, dst) in enumerate(
            [(conv_hbm, conv_ref), (dir_hbm, dir_ref), (outlet_hbm, outlet_ref)]
            + [
                (src.at[:, pl.ds(c * LANES, LANES)], near.at[a, c, pl.ds(0, rows)])
                for a, src in enumerate((depth_hbm, rain_hbm))
                for c in range(own)
            ]
        )
    ]
    for load in loads:
        load.start()
    for load in loads:
        load.wait()

    low = lax.broadcasted_iota(jnp.int32, (SUB, LANES), 1) < HALF

    for c in range(own):
        at = pl.ds(c * LANES, LANES)
        code = dir_ref[:, at]
        near[2, c, pl.ds(0, rows)] = conv_ref[:, at] * jnp.where(
            (code & 1) == 1, f32(0.70710678), f32(1.0)
        )
        near[3, c, pl.ds(0, rows)] = jnp.where(outlet_ref[:, at] == 1, 0, code + 1).astype(f32)

    for a in range(4):
        for c in range(own):
            at = pl.ds((c * 4 + a) * REACH, REACH)
            rows_out[0, at] = near[a, c, pl.ds(0, REACH)]
            rows_out[1, at] = near[a, c, pl.ds(rows - REACH, REACH)]

    def shift_tiles(field, get, blocks):
        for t in range(rows // SUB):
            tile = pl.ds(t * SUB, SUB)
            turned = {}
            for j in blocks:
                for c in (j - 1, j):
                    if c not in turned:
                        turned[c] = pltpu.roll(get(west if c < 0 else c, tile), HALF, 1)
                shifted[field, j, tile] = jnp.where(low, turned[j - 1], turned[j])

    def route_tile(c, tile):
        return near[3, c, tile]

    def near_ends(k):
        dr, dc = OFFSETS[k]
        if dc == 0:
            part = pl.ds(0, 4 * own * REACH)
            src, dst = (
                (rows_out.at[0, part], rows_in.at[1, part])
                if dr < 0
                else (rows_out.at[1, part], rows_in.at[0, part])
            )
        elif dr == 0:
            part = pl.ds(0, rows)
            src = near.at[:, 0 if dc < 0 else own - 1, part]
            dst = near.at[:, east if dc < 0 else west, part]
        else:
            part = pl.ds(0 if dc < 0 else 4 * own * REACH - PACK, PACK)
            src = rows_out.at[0 if dr < 0 else 1, part]
            dst = corners_in.at[k, pl.ds(0, PACK)]
        return src, dst

    def near_copy(k):
        dr, dc = OFFSETS[k]
        src, dst = near_ends(k)
        return pltpu.make_async_remote_copy(
            src_ref=src, dst_ref=dst, send_sem=near_send.at[k], recv_sem=near_recv.at[k],
            device_id=(my_row + dr, my_col + dc), device_id_type=MESH,
        )

    def window_copy(field, half, q):
        peer = lax.rem(my_row + q, row_peers)
        return pltpu.make_async_remote_copy(
            src_ref=shifted.at[field, peer + half],
            dst_ref=window.at[field, half, pl.ds(pl.multiple_of(my_row * rows, rows), rows)],
            send_sem=peer_send.at[field, half, q], recv_sem=peer_recv.at[field, half, q],
            device_id=(peer, my_col), device_id_type=MESH,
        )

    def send_window(field, early, late):
        for q in range(1, row_peers):
            peer = lax.rem(my_row + q, row_peers)
            for half in (0, 1):
                edge = peer == (0, row_peers - 1)[half]
                if early and late:
                    window_copy(field, half, q).start()
                else:
                    @pl.when(edge if late else jnp.logical_not(edge))
                    def _(half=half, q=q):
                        window_copy(field, half, q).start()
        if late:
            window[field, :, pl.ds(pl.multiple_of(my_row * rows, rows), rows)] = shifted[
                field, pl.ds(my_row, 2)
            ]

    def receive_window(field):
        for q in range(1, row_peers):
            for half in (0, 1):
                window_copy(field, half, q).wait_recv()

    def window_sent(field):
        for q in range(1, row_peers):
            for half in (0, 1):
                window_copy(field, half, q).wait_send()

    order = (1, 3, 5, 7, 2, 6, 0, 4)
    pl.semaphore_wait(barrier, expected)
    for k in order:
        @pl.when(exists(*OFFSETS[k]))
        def _(k=k):
            near_copy(k).start()
    shift_tiles(0, route_tile, range(1, own))
    send_window(0, True, False)

    blank = pl.ds(rows + REACH, total - rows - 2 * REACH)
    near[:, :, blank] = jnp.zeros((4, own + 2, total - rows - 2 * REACH, LANES), f32)

    for k in order:
        dr, dc = OFFSETS[k]
        there = exists(-dr, -dc)

        @pl.when(there)
        def _(k=k):
            near_copy(k).wait_recv()

        @pl.when(jnp.logical_not(there))
        def _(k=k):
            dst = near_ends(k)[1]
            dst[...] = jnp.zeros(dst.shape, f32)

    below, above = pl.ds(rows, REACH), pl.ds(total - REACH, REACH)
    for a in range(4):
        for c in range(own):
            at = pl.ds((c * 4 + a) * REACH, REACH)
            near[a, c, below] = rows_in[1, at]
            near[a, c, above] = rows_in[0, at]
        for k in (1, 3, 5, 7):
            dr, dc = OFFSETS[k]
            start = 0 if dc < 0 else PACK - 4 * REACH
            near[a, east if dc < 0 else west, below if dr < 0 else above] = corners_in[
                k, pl.ds(start + a * REACH, REACH)
            ]

    shift_tiles(0, route_tile, (0, own))
    send_window(0, False, True)

    def near_band(a, v):
        take = pl.ds(v, SUB, stride=thin)
        return jnp.concatenate([near[a, c, take, :] for c in range(own + 2)], axis=1)

    for v in range(thin):
        h[v] = near_band(0, v)
        rain[v] = near_band(1, v)
        coef[v] = near_band(2, v)
        base[v] = near_band(3, v)

    def mask_rows(dst, count, up, here, down):
        for v in range(count):
            rows_near = {1: up(v), 0: here(v), -1: down(v)}
            for k, (di, dj) in enumerate(OFFSETS):
                dst[k, v] = jnp.where(rows_near[di] == k + 1, f32(1.0), f32(0.0))

    mask_rows(
        near_masks, thin,
        lambda v: base[v - 1] if v else pltpu.roll(base[thin - 1], 1, 0),
        lambda v: base[v],
        lambda v: base[v + 1] if v < thin - 1 else pltpu.roll(base[0], SUB - 1, 0),
    )

    def sweep(field, mask, count, width, finish):
        start = field[0]
        up, here = pltpu.roll(field[count - 1], 1, 0), start
        for v in range(count):
            down = field[v + 1] if v < count - 1 else pltpu.roll(start, SUB - 1, 0)
            rows_near = {1: up, 0: here, -1: down}
            parts = {}
            for k, (di, dj) in enumerate(OFFSETS):
                term = mask[k, v] * rows_near[di]
                parts[dj] = parts[dj] + term if dj in parts else term
            finish(
                v, parts[0] + (pltpu.roll(parts[1], 1, 1) + pltpu.roll(parts[-1], width - 1, 1))
            )
            up, here = here, down

    @pl.loop(0, SUBSTEPS)
    def _(step):
        for v in range(thin):
            depth = h[v]
            factor = coef[v] * jnp.exp(jnp.log(depth) * f32(2.0 / 3.0))
            out = depth * (factor / (1.0 + factor))
            share[v] = out
            base[v] = depth + rain[v] - out

        def finish(v, came):
            h[v] = base[v] + came

        sweep(share, near_masks, thin, wide, finish)

    for v in range(thin):
        value = h[v]
        for c in range(own + 2):
            plain[c, pl.ds(v, SUB, stride=thin), :] = value[:, c * LANES : (c + 1) * LANES]
    shift_tiles(1, lambda c, tile: plain[c, tile], range(own + 1))
    send_window(1, True, True)
    for c in range(own):
        out_ref[0, :, pl.ds(c * LANES, LANES)] = plain[c, pl.ds(0, rows)]

    def lay(field):
        for b in (0, 1):
            for half in (0, 1):
                tall[b, pl.ds(half * LANES, LANES), :] = window[
                    field, half, pl.ds(b, LANES, stride=2), :
                ].T

    def band(ref, first, count, v, b):
        return ref[b, pl.ds(first + v, SUB, stride=count), :]

    plan = stage_plan()
    along = lax.broadcasted_iota(jnp.int32, (SUB, LANES), 1)
    receive_window(0)
    lay(0)
    for (_, first, count), masks in zip(plan, stage_masks):
        for b in (0, 1):
            codes = [band(tall, first, count, v, b) for v in range(count)]
            for v in range(count):
                cols_near = {
                    1: codes[v - 1] if v else pltpu.roll(codes[-1], 1, 0),
                    0: codes[v],
                    -1: codes[v + 1] if v < count - 1 else pltpu.roll(codes[0], SUB - 1, 0),
                }
                for k, (di, dj) in enumerate(OFFSETS):
                    here = cols_near[dj] == k + 1
                    if (di, b) == (1, 1):
                        here = here & (along < LANES - 1)
                    elif (di, b) == (-1, 0):
                        here = here & (along > 0)
                    masks[k, v, b] = jnp.where(here, f32(1.0), f32(0.0))
    receive_window(1)
    lay(1)

    def pair(ref, v):
        return ref[v, 0], ref[v, 1]

    def turn(values, amount):
        return tuple(pltpu.roll(value, amount, 0) for value in values)

    def gather(held, seed, left, here, right):
        cols_near = {1: left, 0: here, -1: right}
        parts = {}
        for k, (di, dj) in enumerate(OFFSETS):
            for b in (0, 1):
                term = held[k, b] * cols_near[dj][b]
                parts[di, b] = parts[di, b] + term if (di, b) in parts else term
        return (
            seed[0] + (parts[0, 0] + (parts[-1, 1] + pltpu.roll(parts[1, 1], 1, 1))),
            seed[1] + (parts[0, 1] + (parts[1, 0] + pltpu.roll(parts[-1, 0], LANES - 1, 1))),
        )

    def put(ref, v, values):
        ref[v, 0], ref[v, 1] = values

    def run(passes, masks, count):
        def fetch(v):
            return {(k, b): masks[k, v, b] for k in range(len(OFFSETS)) for b in (0, 1)}

        @pl.loop(0, passes // 2)
        def _(index):
            left, here = turn(pair(acc, count - 1), 1), pair(acc, 0)
            older = newer = held = seed = None
            for v in range(count):
                right = pair(acc, v + 1) if v < count - 1 else turn(pair(acc, 0), SUB - 1)
                fresh, start = fetch(v), pair(level, v)
                value = gather(fresh, start, left, here, right)
                if v < 2:
                    put(hold, v, value)
                else:
                    put(acc, v - 1, gather(held, seed, older, newer, value))
                older, newer = newer, value
                held, seed = fresh, start
                left, here = here, right
            put(acc, count - 1, gather(held, seed, older, newer, turn(pair(hold, 0), SUB - 1)))
            put(
                acc, 0,
                gather(fetch(0), pair(level, 0), turn(newer, 1), pair(hold, 0), pair(hold, 1)),
            )

    source = tall
    for (passes, first, count), masks in zip(plan, stage_masks):
        for v in range(count):
            for b in (0, 1):
                value = band(tall, first, count, v, b)
                level[v, b] = value
                acc[v, b] = value if source is tall else band(source, first, count, v, b)
        run(passes, masks, count)
        source = moved
        for v in range(count):
            for b in (0, 1):
                moved[b, pl.ds(first + v, SUB, stride=count), :] = acc[v, b]
    for b in (0, 1):
        core = jnp.log(1.0 + moved[b, pl.ds(HALF, LANES), :])
        result[pl.ds(b, LANES, stride=2), :] = core.T

    mine = pl.ds(pl.multiple_of(my_row * LANES, LANES), LANES)

    def result_copy(q):
        peer = lax.rem(my_row + q, row_peers)
        return pltpu.make_async_remote_copy(
            src_ref=result.at[pl.ds(pl.multiple_of(peer * rows, rows), rows)],
            dst_ref=out_ref.at[1, :, mine],
            send_sem=peer_send.at[2, 0, q], recv_sem=peer_recv.at[2, 0, q],
            device_id=(peer, my_col), device_id_type=MESH,
        )

    for q in range(1, row_peers):
        result_copy(q).start()
    out_ref[1, :, mine] = result[pl.ds(pl.multiple_of(my_row * rows, rows), rows)]
    for k in order:
        @pl.when(exists(*OFFSETS[k]))
        def _(k=k):
            near_copy(k).wait_send()
    window_sent(0)
    window_sent(1)
    for q in range(1, row_peers):
        result_copy(q).wait_recv()
    for q in range(1, row_peers):
        result_copy(q).wait_send()


def strip_call(row_peers, col_peers, rows, cols):
    own = cols // LANES
    total = rows + 2 * SUB
    thin, bands = total // SUB, 2 * LANES // SUB
    f32, i32 = jnp.float32, jnp.int32
    tile = (rows, cols)
    slim = (thin, SUB, cols + 2 * LANES)
    field = (bands, 2, SUB, LANES)
    return pl.pallas_call(
        functools.partial(strip_kernel, row_peers, col_peers),
        out_shape=jax.ShapeDtypeStruct((2, rows, cols), f32),
        in_specs=[pl.BlockSpec(memory_space=pltpu.HBM)] * 5,
        out_specs=pl.BlockSpec(memory_space=pltpu.VMEM),
        scratch_shapes=[
            pltpu.VMEM(tile, f32),
            pltpu.VMEM(tile, i32),
            pltpu.VMEM(tile, i32),
            pltpu.VMEM((4, own + 2, total + SUB, LANES), f32),
            pltpu.VMEM((2, 4 * own * REACH + SUB, LANES), f32),
            pltpu.VMEM((2, 4 * own * REACH + SUB, LANES), f32),
            pltpu.VMEM((len(OFFSETS), PACK + SUB, LANES), f32),
            pltpu.VMEM((own + 2, total, LANES), f32),
            pltpu.VMEM(slim, f32),
            pltpu.VMEM(slim, f32),
            pltpu.VMEM(slim, f32),
            pltpu.VMEM(slim, f32),
            pltpu.VMEM(slim, f32),
            pltpu.VMEM((len(OFFSETS),) + slim, f32),
            pltpu.VMEM((2, own + 1, rows, LANES), f32),
            pltpu.VMEM((2, 2, row_peers * rows, LANES), f32),
            pltpu.VMEM(field, f32),
            pltpu.VMEM(field, f32),
            pltpu.VMEM((2, 2, SUB, LANES), f32),
            pltpu.VMEM((2, 2 * LANES, LANES), f32),
            pltpu.VMEM((2, 2 * LANES, LANES), f32),
            pltpu.VMEM((row_peers * rows, LANES), f32),
            pltpu.SemaphoreType.DMA((3 + 2 * own,)),
            pltpu.SemaphoreType.DMA((len(OFFSETS),)),
            pltpu.SemaphoreType.DMA((len(OFFSETS),)),
            pltpu.SemaphoreType.DMA((3, 2, row_peers)),
            pltpu.SemaphoreType.DMA((3, 2, row_peers)),
        ]
        + [
            pltpu.VMEM((len(OFFSETS), count, 2, SUB, LANES), f32)
            for _, _, count in stage_plan()
        ],
        compiler_params=pltpu.CompilerParams(
            collective_id=0, has_side_effects=True, vmem_limit_bytes=VMEM_BYTES
        ),
    )


def solution(mesh):
    row_peers, col_peers = mesh.shape["row"], mesh.shape["col"]

    def on_device(depth, rainfall, conveyance, flow_dir, outlet):
        rows, cols = depth.shape
        total = rows + 2 * MARGIN + SPARE
        bands = total // SUB
        wide = cols + LANES
        slots = 5 + GROUPS
        own = cols // LANES
        ext = (own + 2, total, LANES)
        field = (bands, SUB, wide)
        vmem = pl.BlockSpec(memory_space=pltpu.VMEM)
        f32 = jnp.float32
        args = tuple(
            pltpu.with_memory_space_constraint(a, pltpu.HBM)
            for a in (depth, rainfall, conveyance, flow_dir, outlet)
        )
        strips = row_peers > 1 and cols == row_peers * LANES and row_peers * rows == 2 * LANES
        if strips and rows % PACK == 0 and row_peers % 2 == 0:
            both = strip_call(row_peers, col_peers, rows, cols)(*args)
            return both[0], both[1]
        hbm = pl.BlockSpec(memory_space=pltpu.HBM)
        tile = (rows, cols)
        both = pl.pallas_call(
            functools.partial(kernel, row_peers, col_peers),
            out_shape=jax.ShapeDtypeStruct((2, rows, cols), f32),
            in_specs=[hbm] * 5,
            out_specs=vmem,
            scratch_shapes=[
                pltpu.VMEM(tile, f32),
                pltpu.VMEM(tile, f32),
                pltpu.VMEM(tile, f32),
                pltpu.VMEM(tile, jnp.int32),
                pltpu.VMEM(tile, jnp.int32),
                pltpu.SemaphoreType.DMA((5,)),
                pltpu.VMEM(ext, f32),
                pltpu.VMEM(ext, f32),
                pltpu.VMEM(ext, f32),
                pltpu.VMEM(ext, jnp.int32),
                pltpu.VMEM(ext, jnp.int32),
                pltpu.VMEM((GROUPS,) + ext, f32),
                pltpu.VMEM((GROUPS + 1, own, total, LANES), f32),
                pltpu.VMEM((GROUPS, len(OFFSETS), SUB, LANES), f32),
                pltpu.VMEM((GROUPS, len(OFFSETS), SUB, LANES), f32),
                pltpu.VMEM(field, f32),
                pltpu.VMEM(field, f32),
                pltpu.VMEM(field, f32),
                pltpu.VMEM(field, f32),
                pltpu.VMEM(field, f32),
                pltpu.VMEM((len(OFFSETS),) + field, f32),
                pltpu.SemaphoreType.DMA((slots, len(OFFSETS))),
                pltpu.SemaphoreType.DMA((slots, len(OFFSETS))),
            ],
            compiler_params=pltpu.CompilerParams(
                collective_id=0, has_side_effects=True, vmem_limit_bytes=VMEM_BYTES
            ),
        )(*args)
        return both[0], both[1]

    placed = P("row", "col")
    return jax.shard_map(
        on_device,
        mesh=mesh,
        in_specs=(placed,) * 5,
        out_specs=(placed, placed),
        check_vma=False,
    )
```

```python
import functools

import jax
import jax.numpy as jnp
from jax import lax
from jax.experimental import pallas as pl
from jax.experimental.pallas import tpu as pltpu
from jax.sharding import PartitionSpec as P

SUBSTEPS = 3
PASSES = 64
OFFSETS = ((0, 1), (1, 1), (1, 0), (1, -1), (0, -1), (-1, -1), (-1, 0), (-1, 1))
LANES = 128
SUB = 8
NEAR = 8
MARGIN = 32
GROUPS = PASSES // MARGIN
SPARE = 0
HALF = LANES // 2
REACH = 3
PACK = 2 * SUB
STAGES = (24, 20, 20)
VMEM_BYTES = 40 * 1024 * 1024
MESH = pl.DeviceIdType.MESH


def kernel(
    row_peers, col_peers,
    depth_hbm, rain_hbm, conv_hbm, dir_hbm, outlet_hbm,
    out_ref,
    depth_ref, rain_ref, conv_ref, dir_ref, outlet_ref, load_sem,
    depth_ext, rain_ext, coef_ext, route_ext, far_ext, acc_ext, plain, pack_out, pack_in,
    acc, rain, coef, level, share, masks,
    send_sem, recv_sem,
):
    rows, cols = depth_ref.shape
    level_ref, discharge_ref = out_ref.at[0], out_ref.at[1]
    total = depth_ext.shape[1]
    bands = total // SUB
    wide = cols + LANES
    own = cols // LANES
    my_row, my_col = lax.axis_index("row"), lax.axis_index("col")

    def exists(dr, dc):
        r, c = my_row + dr, my_col + dc
        ok = None
        for test in ((r >= 0, r < row_peers) if dr else ()) + ((c >= 0, c < col_peers) if dc else ()):
            ok = test if ok is None else jnp.logical_and(ok, test)
        return ok

    def row_place(dr, width):
        if dr == 0:
            return (pl.ds(0, rows), pl.ds(0, rows))
        if dr < 0:
            return (pl.ds(0, width), pl.ds(rows, width))
        return (pl.ds(rows - width, width), pl.ds(total - width, width))

    def col_place(dc):
        if dc == 0:
            return (pl.ds(0, own), pl.ds(0, own))
        if dc < 0:
            return (pl.ds(0, 1), pl.ds(own, 1))
        return (pl.ds(own - 1, 1), pl.ds(own + 1, 1))

    def copy(slot, k, src, dst, width):
        dr, dc = OFFSETS[k]
        (rs, rd), (cs, cd) = row_place(dr, width), col_place(dc)
        return pltpu.make_async_remote_copy(
            src_ref=src.at[cs, rs],
            dst_ref=dst.at[cd, rd],
            send_sem=send_sem.at[slot, k],
            recv_sem=recv_sem.at[slot, k],
            device_id=(my_row + dr, my_col + dc),
            device_id_type=MESH,
        )

    every = (1, 3, 5, 7, 2, 6, 0, 4)
    slanted = (1, 3, 5, 7, 2, 6)
    straight, corners = (2, 6, 0, 4), (1, 3, 5, 7)

    def send(slot, src, dst, width, order=every):
        for k in order:
            @pl.when(exists(*OFFSETS[k]))
            def _(k=k):
                copy(slot, k, src, dst, width).start()

    def receive(slot, src, dst, width, order=every):
        for k in order:
            dr, dc = OFFSETS[k]
            there = exists(-dr, -dc)

            @pl.when(there)
            def _(k=k):
                copy(slot, k, src, dst, width).wait_recv()

            @pl.when(jnp.logical_not(there))
            def _(dr=dr, dc=dc):
                _, rd = row_place(dr, width)
                _, cd = col_place(dc)
                dst[cd, rd] = jnp.zeros((cd.size, rd.size, LANES), dst.dtype)

    def sent_out(slot, src, dst, width, order=every):
        for k in order:
            @pl.when(exists(*OFFSETS[k]))
            def _(k=k):
                copy(slot, k, src, dst, width).wait_send()

    barrier = pltpu.get_barrier_semaphore()
    for dr, dc in OFFSETS:
        @pl.when(exists(dr, dc))
        def _(dr=dr, dc=dc):
            pl.semaphore_signal(
                barrier, inc=1, device_id=(my_row + dr, my_col + dc), device_id_type=MESH
            )
    staged = (
        (depth_hbm, depth_ref), (rain_hbm, rain_ref), (conv_hbm, conv_ref),
        (dir_hbm, dir_ref), (outlet_hbm, outlet_ref),
    )
    loads = [pltpu.make_async_copy(src, dst, load_sem.at[i]) for i, (src, dst) in enumerate(staged)]
    for load in loads:
        load.start()
    for load in loads:
        load.wait()
    for c in range(own):
        at = pl.ds(c * LANES, LANES)
        mine = pl.ds(0, rows)
        depth_ext[c, mine] = depth_ref[:, at]
        rain_ext[c, mine] = rain_ref[:, at]
        code = dir_ref[:, at]
        route = jnp.where(outlet_ref[:, at] == 1, 0, code + 1)
        route_ext[c, mine] = route
        far_ext[c, mine] = route
        coef_ext[c, mine] = conv_ref[:, at] * jnp.where(
            (code & 1) == 1, jnp.float32(0.70710678), jnp.float32(1.0)
        )
    def reach(index, peers):
        return 1 + jnp.where(index > 0, 1, 0) + jnp.where(index < peers - 1, 1, 0)

    pl.semaphore_wait(barrier, reach(my_row, row_peers) * reach(my_col, col_peers) - 1)

    firsts = (depth_ext, coef_ext, rain_ext, route_ext)
    far_slot, level_slot = (len(firsts), len(firsts) + 1)
    for slot, ext in enumerate(firsts):
        send(slot, ext, ext, NEAR)
    send(far_slot, far_ext, far_ext, MARGIN, slanted)
    unused = pl.ds(rows + NEAR, total - rows - 2 * NEAR)
    for ext in firsts:
        ext[:, unused] = jnp.zeros((own + 2, total - rows - 2 * NEAR, LANES), ext.dtype)
    if SPARE:
        for ext in (far_ext,) + tuple(acc_ext.at[g] for g in range(GROUPS)):
            ext[:, pl.ds(rows + MARGIN, SPARE)] = jnp.zeros((own + 2, SPARE, LANES), ext.dtype)
    for slot, ext in enumerate(firsts):
        receive(slot, ext, ext, NEAR)
    sides = (pl.ds(own, 2), pl.ds(0, rows))
    far_ext[sides] = route_ext[sides]

    right = lax.broadcasted_iota(jnp.int32, (SUB, LANES), 1) < LANES // 2

    def banded(ext, v):
        def part(c):
            return ext[c, pl.ds(v, SUB, stride=bands), :]

        blocks = [part(c) for c in range(own)]
        blocks.append(jnp.where(right, part(own), part(own + 1)))
        return jnp.concatenate(blocks, axis=1)

    for v in range(bands):
        acc[v] = banded(depth_ext, v)
        rain[v] = banded(rain_ext, v)
        coef[v] = banded(coef_ext, v)

    def above(v, get):
        return get(v - 1) if v else pltpu.roll(get(bands - 1), 1, 0)

    def below(v, get):
        return get(v + 1) if v < bands - 1 else pltpu.roll(get(0), SUB - 1, 0)

    def set_masks(ext):
        def routed(v):
            return banded(ext, v)

        for v in range(bands):
            near = {1: above(v, routed), 0: routed(v), -1: below(v, routed)}
            for k, (di, dj) in enumerate(OFFSETS):
                masks[k, v] = jnp.where(near[di] == k + 1, jnp.float32(1.0), jnp.float32(0.0))

    set_masks(route_ext)

    def inflow(v, up, here, down):
        near = {1: up, 0: here, -1: down}
        parts = {}
        for k, (di, dj) in enumerate(OFFSETS):
            term = masks[k, v] * near[di]
            parts[dj] = parts[dj] + term if dj in parts else term
        return parts[0] + (pltpu.roll(parts[1], 1, 1) + pltpu.roll(parts[-1], wide - 1, 1))

    def sweep(field, finish):
        start = field[0]
        up, here = (pltpu.roll(field[bands - 1], 1, 0), start)
        for v in range(bands):
            down = field[v + 1] if v < bands - 1 else pltpu.roll(start, SUB - 1, 0)
            finish(v, inflow(v, up, here, down))
            up, here = here, down

    @pl.loop(0, SUBSTEPS)
    def _(step):
        for v in range(bands):
            h = acc[v]
            factor = coef[v] * jnp.exp(jnp.log(h) * jnp.float32(2.0 / 3.0))
            out = h * (factor / (1.0 + factor))
            share[v] = out
            level[v] = h + rain[v] - out

        def finish(v, came):
            acc[v] = level[v] + came

        sweep(share, finish)

    def finish(v, came):
        acc[v] = level[v] + came

    def passes(count):
        @pl.loop(0, count)
        def _(index):
            sweep(acc, finish)

    def to_plain(field, dst):
        for v in range(bands):
            value = field[v]
            for c in range(own):
                dst[c, pl.ds(v, SUB, stride=bands), :] = value[:, c * LANES : (c + 1) * LANES]

    sub = lax.broadcasted_iota(jnp.int32, (SUB, LANES), 0)

    lane_part = lax.broadcasted_iota(jnp.int32, (SUB, LANES), 1) // MARGIN

    def corner(group, k):
        dr, dc = OFFSETS[k]
        slot = level_slot + group
        return pltpu.make_async_remote_copy(
            src_ref=pack_out.at[group, k],
            dst_ref=pack_in.at[group, k],
            send_sem=send_sem.at[slot, k],
            recv_sem=recv_sem.at[slot, k],
            device_id=(my_row + dr, my_col + dc),
            device_id_type=MESH,
        )

    def send_corners(group, src):
        for k in corners:
            dr, dc = OFFSETS[k]
            start = 0 if dr < 0 else rows - MARGIN
            block, first = (0, 0) if dc < 0 else (own - 1, LANES - MARGIN)
            packed = None
            for g in range(MARGIN // SUB):
                piece = src[block, pl.ds(start + g * SUB, SUB), :]
                shift = (g * MARGIN - first) % LANES
                piece = pltpu.roll(piece, shift, 1) if shift else piece
                packed = piece if packed is None else jnp.where(lane_part == g, piece, packed)
            pack_out[group, k] = packed
        for k in corners:
            @pl.when(exists(*OFFSETS[k]))
            def _(k=k):
                corner(group, k).start()

    def receive_corners(group, dst):
        for k in corners:
            dr, dc = OFFSETS[k]
            there = exists(-dr, -dc)
            start = rows if dr < 0 else total - MARGIN
            block, first = (own, 0) if dc < 0 else (own + 1, LANES - MARGIN)

            @pl.when(there)
            def _(k=k, start=start, block=block, first=first):
                corner(group, k).wait_recv()
                packed = pack_in[group, k]
                for g in range(MARGIN // SUB):
                    shift = (first - g * MARGIN) % LANES
                    piece = pltpu.roll(packed, shift, 1) if shift else packed
                    dst[block, pl.ds(start + g * SUB, SUB), :] = piece

            @pl.when(jnp.logical_not(there))
            def _(start=start, block=block):
                dst[block, pl.ds(start, MARGIN), :] = jnp.zeros((MARGIN, LANES), dst.dtype)

    def widen(src, dst, group, meanwhile, fields):
        slot = level_slot + group
        to_plain(acc, src)
        send_corners(group, src)
        send(slot, src, dst, MARGIN, straight)
        meanwhile()
        receive(slot, src, dst, MARGIN, straight)
        receive_corners(group, dst)
        for v in range(bands):
            inner = sub * bands + v < rows
            for c in range(own):
                at = pl.ds(c * LANES, LANES)
                value = jnp.where(inner, acc[v, :, at], dst[c, pl.ds(v, SUB, stride=bands), :])
                for field in fields:
                    field[v, :, at] = value
            value = jnp.where(
                right,
                dst[own, pl.ds(v, SUB, stride=bands), :],
                dst[own + 1, pl.ds(v, SUB, stride=bands), :],
            )
            for field in fields:
                field[v, :, pl.ds(cols, LANES)] = value

    def in_flight():
        for c in range(own):
            level_ref[:, pl.ds(c * LANES, LANES)] = plain[0, c, pl.ds(0, rows), :]
        receive(far_slot, far_ext, far_ext, MARGIN, slanted)
        set_masks(far_ext)

    widen(plain.at[0], acc_ext.at[0], 0, in_flight, (acc, level))
    passes(MARGIN)
    for group in range(1, GROUPS):
        widen(plain.at[group], acc_ext.at[group], group, lambda: None, (acc,))
        passes(MARGIN)

    to_plain(acc, plain.at[GROUPS])
    for c in range(own):
        discharge_ref[:, pl.ds(c * LANES, LANES)] = jnp.log(1.0 + plain[GROUPS, c, pl.ds(0, rows), :])
    for slot, ext in enumerate(firsts):
        sent_out(slot, ext, ext, NEAR)
    sent_out(far_slot, far_ext, far_ext, MARGIN, slanted)
    for group in range(GROUPS):
        sent_out(level_slot + group, plain.at[group], acc_ext.at[group], MARGIN, straight)
        for k in corners:
            @pl.when(exists(*OFFSETS[k]))
            def _(group=group, k=k):
                corner(group, k).wait_send()


def stage_plan():
    left, plan = PASSES, []
    for count in STAGES:
        plan.append((count, HALF - left, (LANES + 2 * left) // SUB))
        left -= count
    return plan


def strip_kernel(
    row_peers, col_peers,
    depth_hbm, rain_hbm, conv_hbm, dir_hbm, outlet_hbm,
    out_ref,
    conv_ref, dir_ref, outlet_ref,
    near, sides_in, rows_out, rows_in, corners_in, plain,
    h, rain, coef, base, share, near_masks,
    shifted, window,
    acc, level, hold, tall, moved, result,
    load_sem, near_send, near_recv, peer_send, peer_recv, rim_send, rim_recv,
    *stage_masks,
):
    rows, cols = conv_ref.shape
    own = cols // LANES
    total = plain.shape[1]
    thin = total // SUB
    east, west = own, own + 1
    wide = cols + 2 * LANES
    f32 = jnp.float32
    my_row, my_col = lax.axis_index("row"), lax.axis_index("col")

    def exists(dr, dc):
        r, c = my_row + dr, my_col + dc
        return (r >= 0) & (r < row_peers) & (c >= 0) & (c < col_peers)

    barrier = pltpu.get_barrier_semaphore()

    def greet(row, col):
        pl.semaphore_signal(barrier, inc=1, device_id=(row, col), device_id_type=MESH)

    expected = row_peers - 1
    for dr, dc in OFFSETS:
        @pl.when(exists(dr, dc))
        def _(dr=dr, dc=dc):
            greet(my_row + dr, my_col + dc)
        if dc:
            expected = expected + jnp.where(exists(dr, dc), 1, 0)
    for q in range(row_peers):
        far = (my_row - q >= 2) | (q - my_row >= 2)

        @pl.when(far)
        def _(q=q):
            greet(q, my_col)

    loads = [
        pltpu.make_async_copy(src, dst, load_sem.at[i])
        for i, (src, dst) in enumerate(
            [(conv_hbm, conv_ref), (dir_hbm, dir_ref), (outlet_hbm, outlet_ref)]
            + [
                (src.at[:, pl.ds(c * LANES, LANES)], near.at[a, c, pl.ds(0, rows)])
                for a, src in enumerate((depth_hbm, rain_hbm))
                for c in range(own)
            ]
        )
    ]
    for load in loads:
        load.start()
    for load in loads:
        load.wait()

    low = lax.broadcasted_iota(jnp.int32, (SUB, LANES), 1) < HALF

    for c in range(own):
        at = pl.ds(c * LANES, LANES)
        code = dir_ref[:, at]
        near[2, c, pl.ds(0, rows)] = conv_ref[:, at] * jnp.where(
            (code & 1) == 1, f32(0.70710678), f32(1.0)
        )
        near[3, c, pl.ds(0, rows)] = jnp.where(outlet_ref[:, at] == 1, 0, code + 1).astype(f32)

    for a in range(4):
        for c in range(own):
            at = pl.ds((c * 4 + a) * REACH, REACH)
            rows_out[0, at] = near[a, c, pl.ds(0, REACH)]
            rows_out[1, at] = near[a, c, pl.ds(rows - REACH, REACH)]

    every = range(rows // SUB)
    rim = (0, rows // SUB - 1)
    inner = range(1, rows // SUB - 1)

    def shift_tiles(field, get, blocks, tiles=every):
        for t in tiles:
            tile = pl.ds(t * SUB, SUB)
            turned = {}
            for j in blocks:
                for c in (j - 1, j):
                    if c not in turned:
                        turned[c] = pltpu.roll(get(west if c < 0 else c, tile), HALF, 1)
                shifted[field, j, tile] = jnp.where(low, turned[j - 1], turned[j])

    def route_tile(c, tile):
        return near[3, c, tile]

    def near_ends(k):
        dr, dc = OFFSETS[k]
        if dc == 0:
            part = pl.ds(0, 4 * own * REACH)
            src, dst = (
                (rows_out.at[0, part], rows_in.at[1, part])
                if dr < 0
                else (rows_out.at[1, part], rows_in.at[0, part])
            )
        elif dr == 0:
            part = pl.ds(0, rows)
            src = near.at[pl.ds(0, 3), 0 if dc < 0 else own - 1, part]
            dst = sides_in.at[0 if dc < 0 else 1, pl.ds(0, 3)]
        else:
            part = pl.ds(0 if dc < 0 else 4 * own * REACH - PACK, PACK)
            src = rows_out.at[0 if dr < 0 else 1, part]
            dst = corners_in.at[k, pl.ds(0, PACK)]
        return src, dst

    def near_copy(k):
        dr, dc = OFFSETS[k]
        src, dst = near_ends(k)
        return pltpu.make_async_remote_copy(
            src_ref=src, dst_ref=dst, send_sem=near_send.at[k], recv_sem=near_recv.at[k],
            device_id=(my_row + dr, my_col + dc), device_id_type=MESH,
        )

    def side_copy(side):
        return pltpu.make_async_remote_copy(
            src_ref=near.at[3, (0, own - 1)[side], pl.ds(0, rows)],
            dst_ref=sides_in.at[side, 3],
            send_sem=near_send.at[len(OFFSETS) + side], recv_sem=near_recv.at[len(OFFSETS) + side],
            device_id=(my_row, my_col + (-1, 1)[side]), device_id_type=MESH,
        )

    def window_copy(field, half, q):
        peer = lax.rem(my_row + q, row_peers)
        return pltpu.make_async_remote_copy(
            src_ref=shifted.at[field, peer + half],
            dst_ref=window.at[field, half, pl.ds(pl.multiple_of(my_row * rows, rows), rows)],
            send_sem=peer_send.at[field, half, q], recv_sem=peer_recv.at[field, half, q],
            device_id=(peer, my_col), device_id_type=MESH,
        )

    def part_copy(half, q, piece):
        peer = lax.rem(my_row + q, row_peers)
        start, size = ((SUB, rows - 2 * SUB), (0, SUB), (rows - SUB, SUB))[piece]
        send, recv = (peer_send, peer_recv) if piece == 0 else (rim_send, rim_recv)
        at = (1, half, q) if piece == 0 else (piece - 1, half, q)
        return pltpu.make_async_remote_copy(
            src_ref=shifted.at[1, peer + half, pl.ds(start, size)],
            dst_ref=window.at[1, half, pl.ds(pl.multiple_of(my_row * rows + start, SUB), size)],
            send_sem=send.at[at], recv_sem=recv.at[at],
            device_id=(peer, my_col), device_id_type=MESH,
        )

    def place(field):
        window[field, :, pl.ds(pl.multiple_of(my_row * rows, rows), rows)] = shifted[
            field, pl.ds(my_row, 2)
        ]

    def each(target, act):
        for q in range(1, row_peers):
            for half in (0, 1):
                row = lax.rem(my_row + q, row_peers) if target else my_row
                act(half, q, row == (0, row_peers - 1)[half])

    def send_route(late):
        def act(half, q, edge):
            @pl.when(edge if late else jnp.logical_not(edge))
            def _():
                window_copy(0, half, q).start()

        each(True, act)

    def send_inner():
        def act(half, q, edge):
            @pl.when(jnp.logical_not(edge))
            def _():
                part_copy(half, q, 0).start()

        each(True, act)

    def send_rest():
        def act(half, q, edge):
            @pl.when(edge)
            def _():
                window_copy(1, half, q).start()

            @pl.when(jnp.logical_not(edge))
            def _():
                part_copy(half, q, 1).start()
                part_copy(half, q, 2).start()

        each(True, act)

    def receive_level():
        def act(half, q, edge):
            @pl.when(edge)
            def _():
                window_copy(1, half, q).wait_recv()

            @pl.when(jnp.logical_not(edge))
            def _():
                for piece in range(3):
                    part_copy(half, q, piece).wait_recv()

        each(False, act)

    def level_sent():
        def act(half, q, edge):
            @pl.when(edge)
            def _():
                window_copy(1, half, q).wait_send()

            @pl.when(jnp.logical_not(edge))
            def _():
                for piece in range(3):
                    part_copy(half, q, piece).wait_send()

        each(True, act)

    def receive_window(field):
        for q in range(1, row_peers):
            for half in (0, 1):
                window_copy(field, half, q).wait_recv()

    def window_sent(field):
        for q in range(1, row_peers):
            for half in (0, 1):
                window_copy(field, half, q).wait_send()

    order = (1, 3, 5, 7, 2, 6, 0, 4)
    pl.semaphore_wait(barrier, expected)
    for side, dc in enumerate((-1, 1)):
        @pl.when(exists(0, dc))
        def _(side=side):
            side_copy(side).start()
    for k in order:
        @pl.when(exists(*OFFSETS[k]))
        def _(k=k):
            near_copy(k).start()
    shift_tiles(0, route_tile, range(1, own))
    send_route(False)

    near[:, pl.ds(0, own), pl.ds(rows, total - rows)] = jnp.zeros((4, own, total - rows, LANES), f32)
    near[:, pl.ds(own, 2), pl.ds(0, total)] = jnp.zeros((4, 2, total, LANES), f32)

    def near_band(a, v):
        take = pl.ds(v, SUB, stride=thin)
        return jnp.concatenate([near[a, c, take, :] for c in range(own + 2)], axis=1)

    def mask_rows(dst, count, up, here, down):
        for v in range(count):
            rows_near = {1: up(v), 0: here(v), -1: down(v)}
            for k, (di, dj) in enumerate(OFFSETS):
                dst[k, v] = jnp.where(rows_near[di] == k + 1, f32(1.0), f32(0.0))

    def sweep(field, mask, count, width, finish):
        start = field[0]
        up, here = pltpu.roll(field[count - 1], 1, 0), start
        for v in range(count):
            down = field[v + 1] if v < count - 1 else pltpu.roll(start, SUB - 1, 0)
            rows_near = {1: up, 0: here, -1: down}
            parts = {}
            for k, (di, dj) in enumerate(OFFSETS):
                term = mask[k, v] * rows_near[di]
                parts[dj] = parts[dj] + term if dj in parts else term
            finish(
                v, parts[0] + (pltpu.roll(parts[1], 1, 1) + pltpu.roll(parts[-1], width - 1, 1))
            )
            up, here = here, down

    def levels():
        for v in range(thin):
            h[v] = near_band(0, v)
            rain[v] = near_band(1, v)
            coef[v] = near_band(2, v)
            base[v] = near_band(3, v)

        mask_rows(
            near_masks, thin,
            lambda v: base[v - 1] if v else pltpu.roll(base[thin - 1], 1, 0),
            lambda v: base[v],
            lambda v: base[v + 1] if v < thin - 1 else pltpu.roll(base[0], SUB - 1, 0),
        )

        @pl.loop(0, SUBSTEPS)
        def _(step):
            for v in range(thin):
                depth = h[v]
                factor = coef[v] * jnp.exp(jnp.log(depth) * f32(2.0 / 3.0))
                out = depth * (factor / (1.0 + factor))
                share[v] = out
                base[v] = depth + rain[v] - out

            def finish(v, came):
                h[v] = base[v] + came

            sweep(share, near_masks, thin, wide, finish)

        for v in range(thin):
            value = h[v]
            for c in range(own + 2):
                plain[c, pl.ds(v, SUB, stride=thin), :] = value[:, c * LANES : (c + 1) * LANES]

    def level_tile(c, tile):
        return plain[c, tile]

    levels()
    shift_tiles(1, level_tile, range(1, own), inner)
    send_inner()
    for side, dc in enumerate((-1, 1)):
        there = exists(0, -dc)

        @pl.when(there)
        def _(side=side):
            side_copy(side).wait_recv()

        @pl.when(jnp.logical_not(there))
        def _(side=side):
            sides_in[side, 3] = jnp.zeros((rows, LANES), f32)

        near[3, own + side, pl.ds(0, rows)] = sides_in[side, 3]
    shift_tiles(0, route_tile, (0, own))
    send_route(True)
    place(0)
    for k in order:
        dr, dc = OFFSETS[k]
        there = exists(-dr, -dc)

        @pl.when(there)
        def _(k=k):
            near_copy(k).wait_recv()

        @pl.when(jnp.logical_not(there))
        def _(k=k):
            dst = near_ends(k)[1]
            dst[...] = jnp.zeros(dst.shape, f32)

    below, above = pl.ds(rows, REACH), pl.ds(total - REACH, REACH)
    for a in range(4):
        for c in range(own):
            at = pl.ds((c * 4 + a) * REACH, REACH)
            near[a, c, below] = rows_in[1, at]
            near[a, c, above] = rows_in[0, at]
        for k in (1, 3, 5, 7):
            dr, dc = OFFSETS[k]
            start = 0 if dc < 0 else PACK - 4 * REACH
            near[a, east if dc < 0 else west, below if dr < 0 else above] = corners_in[
                k, pl.ds(start + a * REACH, REACH)
            ]

    for side in (0, 1):
        near[pl.ds(0, 3), own + side, pl.ds(0, rows)] = sides_in[side, pl.ds(0, 3)]

    levels()
    shift_tiles(1, level_tile, (0, own))
    shift_tiles(1, level_tile, range(1, own), rim)
    send_rest()
    place(1)
    for c in range(own):
        out_ref[0, :, pl.ds(c * LANES, LANES)] = plain[c, pl.ds(0, rows)]

    def lay(field):
        for b in (0, 1):
            for half in (0, 1):
                tall[b, pl.ds(half * LANES, LANES), :] = window[
                    field, half, pl.ds(b, LANES, stride=2), :
                ].T

    def band(ref, first, count, v, b):
        return ref[b, pl.ds(first + v, SUB, stride=count), :]

    plan = stage_plan()
    along = lax.broadcasted_iota(jnp.int32, (SUB, LANES), 1)
    receive_window(0)
    lay(0)
    for (_, first, count), masks in zip(plan, stage_masks):
        for b in (0, 1):
            codes = [band(tall, first, count, v, b) for v in range(count)]
            for v in range(count):
                cols_near = {
                    1: codes[v - 1] if v else pltpu.roll(codes[-1], 1, 0),
                    0: codes[v],
                    -1: codes[v + 1] if v < count - 1 else pltpu.roll(codes[0], SUB - 1, 0),
                }
                for k, (di, dj) in enumerate(OFFSETS):
                    here = cols_near[dj] == k + 1
                    if (di, b) == (1, 1):
                        here = here & (along < LANES - 1)
                    elif (di, b) == (-1, 0):
                        here = here & (along > 0)
                    masks[k, v, b] = jnp.where(here, f32(1.0), f32(0.0))
    receive_level()
    lay(1)

    def pair(ref, v):
        return ref[v, 0], ref[v, 1]

    def turn(values, amount):
        return tuple(pltpu.roll(value, amount, 0) for value in values)

    def gather(held, seed, left, here, right):
        cols_near = {1: left, 0: here, -1: right}
        parts = {}
        for k, (di, dj) in enumerate(OFFSETS):
            for b in (0, 1):
                term = held[k, b] * cols_near[dj][b]
                parts[di, b] = parts[di, b] + term if (di, b) in parts else term
        return (
            seed[0] + (parts[0, 0] + (parts[-1, 1] + pltpu.roll(parts[1, 1], 1, 1))),
            seed[1] + (parts[0, 1] + (parts[1, 0] + pltpu.roll(parts[-1, 0], LANES - 1, 1))),
        )

    def put(ref, v, values):
        ref[v, 0], ref[v, 1] = values

    def run(passes, masks, count):
        def fetch(v):
            return {(k, b): masks[k, v, b] for k in range(len(OFFSETS)) for b in (0, 1)}

        @pl.loop(0, passes // 2)
        def _(index):
            left, here = turn(pair(acc, count - 1), 1), pair(acc, 0)
            older = newer = held = seed = None
            for v in range(count):
                right = pair(acc, v + 1) if v < count - 1 else turn(pair(acc, 0), SUB - 1)
                fresh, start = fetch(v), pair(level, v)
                value = gather(fresh, start, left, here, right)
                if v < 2:
                    put(hold, v, value)
                else:
                    put(acc, v - 1, gather(held, seed, older, newer, value))
                older, newer = newer, value
                held, seed = fresh, start
                left, here = here, right
            put(acc, count - 1, gather(held, seed, older, newer, turn(pair(hold, 0), SUB - 1)))
            put(
                acc, 0,
                gather(fetch(0), pair(level, 0), turn(newer, 1), pair(hold, 0), pair(hold, 1)),
            )

    source = tall
    for (passes, first, count), masks in zip(plan, stage_masks):
        for v in range(count):
            for b in (0, 1):
                value = band(tall, first, count, v, b)
                level[v, b] = value
                acc[v, b] = value if source is tall else band(source, first, count, v, b)
        run(passes, masks, count)
        source = moved
        for v in range(count):
            for b in (0, 1):
                moved[b, pl.ds(first + v, SUB, stride=count), :] = acc[v, b]
    for b in (0, 1):
        core = jnp.log(1.0 + moved[b, pl.ds(HALF, LANES), :])
        result[pl.ds(b, LANES, stride=2), :] = core.T

    mine = pl.ds(pl.multiple_of(my_row * LANES, LANES), LANES)

    def result_copy(q):
        peer = lax.rem(my_row + q, row_peers)
        return pltpu.make_async_remote_copy(
            src_ref=result.at[pl.ds(pl.multiple_of(peer * rows, rows), rows)],
            dst_ref=out_ref.at[1, :, mine],
            send_sem=peer_send.at[2, 0, q], recv_sem=peer_recv.at[2, 0, q],
            device_id=(peer, my_col), device_id_type=MESH,
        )

    for q in range(1, row_peers):
        result_copy(q).start()
    out_ref[1, :, mine] = result[pl.ds(pl.multiple_of(my_row * rows, rows), rows)]
    for k in order:
        @pl.when(exists(*OFFSETS[k]))
        def _(k=k):
            near_copy(k).wait_send()
    for side, dc in enumerate((-1, 1)):
        @pl.when(exists(0, dc))
        def _(side=side):
            side_copy(side).wait_send()
    window_sent(0)
    level_sent()
    for q in range(1, row_peers):
        result_copy(q).wait_recv()
    for q in range(1, row_peers):
        result_copy(q).wait_send()


def strip_call(row_peers, col_peers, rows, cols):
    own = cols // LANES
    total = rows + 2 * SUB
    thin, bands = total // SUB, 2 * LANES // SUB
    f32, i32 = jnp.float32, jnp.int32
    tile = (rows, cols)
    slim = (thin, SUB, cols + 2 * LANES)
    field = (bands, 2, SUB, LANES)
    return pl.pallas_call(
        functools.partial(strip_kernel, row_peers, col_peers),
        out_shape=jax.ShapeDtypeStruct((2, rows, cols), f32),
        in_specs=[pl.BlockSpec(memory_space=pltpu.HBM)] * 5,
        out_specs=pl.BlockSpec(memory_space=pltpu.VMEM),
        scratch_shapes=[
            pltpu.VMEM(tile, f32),
            pltpu.VMEM(tile, i32),
            pltpu.VMEM(tile, i32),
            pltpu.VMEM((4, own + 2, total + SUB, LANES), f32),
            pltpu.VMEM((2, 4, rows, LANES), f32),
            pltpu.VMEM((2, 4 * own * REACH + SUB, LANES), f32),
            pltpu.VMEM((2, 4 * own * REACH + SUB, LANES), f32),
            pltpu.VMEM((len(OFFSETS), PACK + SUB, LANES), f32),
            pltpu.VMEM((own + 2, total, LANES), f32),
            pltpu.VMEM(slim, f32),
            pltpu.VMEM(slim, f32),
            pltpu.VMEM(slim, f32),
            pltpu.VMEM(slim, f32),
            pltpu.VMEM(slim, f32),
            pltpu.VMEM((len(OFFSETS),) + slim, f32),
            pltpu.VMEM((2, own + 1, rows, LANES), f32),
            pltpu.VMEM((2, 2, row_peers * rows, LANES), f32),
            pltpu.VMEM(field, f32),
            pltpu.VMEM(field, f32),
            pltpu.VMEM((2, 2, SUB, LANES), f32),
            pltpu.VMEM((2, 2 * LANES, LANES), f32),
            pltpu.VMEM((2, 2 * LANES, LANES), f32),
            pltpu.VMEM((row_peers * rows, LANES), f32),
            pltpu.SemaphoreType.DMA((3 + 2 * own,)),
            pltpu.SemaphoreType.DMA((len(OFFSETS) + 2,)),
            pltpu.SemaphoreType.DMA((len(OFFSETS) + 2,)),
            pltpu.SemaphoreType.DMA((3, 2, row_peers)),
            pltpu.SemaphoreType.DMA((3, 2, row_peers)),
            pltpu.SemaphoreType.DMA((2, 2, row_peers)),
            pltpu.SemaphoreType.DMA((2, 2, row_peers)),
        ]
        + [
            pltpu.VMEM((len(OFFSETS), count, 2, SUB, LANES), f32)
            for _, _, count in stage_plan()
        ],
        compiler_params=pltpu.CompilerParams(
            collective_id=0, has_side_effects=True, vmem_limit_bytes=VMEM_BYTES
        ),
    )


def solution(mesh):
    row_peers, col_peers = mesh.shape["row"], mesh.shape["col"]

    def on_device(depth, rainfall, conveyance, flow_dir, outlet):
        rows, cols = depth.shape
        total = rows + 2 * MARGIN + SPARE
        bands = total // SUB
        wide = cols + LANES
        slots = 5 + GROUPS
        own = cols // LANES
        ext = (own + 2, total, LANES)
        field = (bands, SUB, wide)
        vmem = pl.BlockSpec(memory_space=pltpu.VMEM)
        f32 = jnp.float32
        args = tuple(
            pltpu.with_memory_space_constraint(a, pltpu.HBM)
            for a in (depth, rainfall, conveyance, flow_dir, outlet)
        )
        strips = row_peers > 1 and cols == row_peers * LANES and row_peers * rows == 2 * LANES
        if strips and rows % PACK == 0 and row_peers % 2 == 0:
            both = strip_call(row_peers, col_peers, rows, cols)(*args)
            return both[0], both[1]
        hbm = pl.BlockSpec(memory_space=pltpu.HBM)
        tile = (rows, cols)
        both = pl.pallas_call(
            functools.partial(kernel, row_peers, col_peers),
            out_shape=jax.ShapeDtypeStruct((2, rows, cols), f32),
            in_specs=[hbm] * 5,
            out_specs=vmem,
            scratch_shapes=[
                pltpu.VMEM(tile, f32),
                pltpu.VMEM(tile, f32),
                pltpu.VMEM(tile, f32),
                pltpu.VMEM(tile, jnp.int32),
                pltpu.VMEM(tile, jnp.int32),
                pltpu.SemaphoreType.DMA((5,)),
                pltpu.VMEM(ext, f32),
                pltpu.VMEM(ext, f32),
                pltpu.VMEM(ext, f32),
                pltpu.VMEM(ext, jnp.int32),
                pltpu.VMEM(ext, jnp.int32),
                pltpu.VMEM((GROUPS,) + ext, f32),
                pltpu.VMEM((GROUPS + 1, own, total, LANES), f32),
                pltpu.VMEM((GROUPS, len(OFFSETS), SUB, LANES), f32),
                pltpu.VMEM((GROUPS, len(OFFSETS), SUB, LANES), f32),
                pltpu.VMEM(field, f32),
                pltpu.VMEM(field, f32),
                pltpu.VMEM(field, f32),
                pltpu.VMEM(field, f32),
                pltpu.VMEM(field, f32),
                pltpu.VMEM((len(OFFSETS),) + field, f32),
                pltpu.SemaphoreType.DMA((slots, len(OFFSETS))),
                pltpu.SemaphoreType.DMA((slots, len(OFFSETS))),
            ],
            compiler_params=pltpu.CompilerParams(
                collective_id=0, has_side_effects=True, vmem_limit_bytes=VMEM_BYTES
            ),
        )(*args)
        return both[0], both[1]

    placed = P("row", "col")
    return jax.shard_map(
        on_device,
        mesh=mesh,
        in_specs=(placed,) * 5,
        out_specs=(placed, placed),
        check_vma=False,
    )
```

```python
import functools

import jax
import jax.numpy as jnp
from jax import lax
from jax.experimental import pallas as pl
from jax.experimental.pallas import tpu as pltpu
from jax.sharding import PartitionSpec as P

SUBSTEPS = 3
PASSES = 64
OFFSETS = ((0, 1), (1, 1), (1, 0), (1, -1), (0, -1), (-1, -1), (-1, 0), (-1, 1))
LANES = 128
SUB = 8
NEAR = 8
MARGIN = 32
GROUPS = PASSES // MARGIN
SPARE = 0
HALF = LANES // 2
REACH = 3
PACK = 2 * SUB
STAGES = (16, 16, 16, 16)
VMEM_BYTES = 40 * 1024 * 1024
MESH = pl.DeviceIdType.MESH


def kernel(
    row_peers, col_peers,
    depth_hbm, rain_hbm, conv_hbm, dir_hbm, outlet_hbm,
    out_ref,
    depth_ref, rain_ref, conv_ref, dir_ref, outlet_ref, load_sem,
    depth_ext, rain_ext, coef_ext, route_ext, far_ext, acc_ext, plain, pack_out, pack_in,
    acc, rain, coef, level, share, masks,
    send_sem, recv_sem,
):
    rows, cols = depth_ref.shape
    level_ref, discharge_ref = out_ref.at[0], out_ref.at[1]
    total = depth_ext.shape[1]
    bands = total // SUB
    wide = cols + LANES
    own = cols // LANES
    my_row, my_col = lax.axis_index("row"), lax.axis_index("col")

    def exists(dr, dc):
        r, c = my_row + dr, my_col + dc
        ok = None
        for test in ((r >= 0, r < row_peers) if dr else ()) + ((c >= 0, c < col_peers) if dc else ()):
            ok = test if ok is None else jnp.logical_and(ok, test)
        return ok

    def row_place(dr, width):
        if dr == 0:
            return (pl.ds(0, rows), pl.ds(0, rows))
        if dr < 0:
            return (pl.ds(0, width), pl.ds(rows, width))
        return (pl.ds(rows - width, width), pl.ds(total - width, width))

    def col_place(dc):
        if dc == 0:
            return (pl.ds(0, own), pl.ds(0, own))
        if dc < 0:
            return (pl.ds(0, 1), pl.ds(own, 1))
        return (pl.ds(own - 1, 1), pl.ds(own + 1, 1))

    def copy(slot, k, src, dst, width):
        dr, dc = OFFSETS[k]
        (rs, rd), (cs, cd) = row_place(dr, width), col_place(dc)
        return pltpu.make_async_remote_copy(
            src_ref=src.at[cs, rs],
            dst_ref=dst.at[cd, rd],
            send_sem=send_sem.at[slot, k],
            recv_sem=recv_sem.at[slot, k],
            device_id=(my_row + dr, my_col + dc),
            device_id_type=MESH,
        )

    every = (1, 3, 5, 7, 2, 6, 0, 4)
    slanted = (1, 3, 5, 7, 2, 6)
    straight, corners = (2, 6, 0, 4), (1, 3, 5, 7)

    def send(slot, src, dst, width, order=every):
        for k in order:
            @pl.when(exists(*OFFSETS[k]))
            def _(k=k):
                copy(slot, k, src, dst, width).start()

    def receive(slot, src, dst, width, order=every):
        for k in order:
            dr, dc = OFFSETS[k]
            there = exists(-dr, -dc)

            @pl.when(there)
            def _(k=k):
                copy(slot, k, src, dst, width).wait_recv()

            @pl.when(jnp.logical_not(there))
            def _(dr=dr, dc=dc):
                _, rd = row_place(dr, width)
                _, cd = col_place(dc)
                dst[cd, rd] = jnp.zeros((cd.size, rd.size, LANES), dst.dtype)

    def sent_out(slot, src, dst, width, order=every):
        for k in order:
            @pl.when(exists(*OFFSETS[k]))
            def _(k=k):
                copy(slot, k, src, dst, width).wait_send()

    barrier = pltpu.get_barrier_semaphore()
    for dr, dc in OFFSETS:
        @pl.when(exists(dr, dc))
        def _(dr=dr, dc=dc):
            pl.semaphore_signal(
                barrier, inc=1, device_id=(my_row + dr, my_col + dc), device_id_type=MESH
            )
    staged = (
        (depth_hbm, depth_ref), (rain_hbm, rain_ref), (conv_hbm, conv_ref),
        (dir_hbm, dir_ref), (outlet_hbm, outlet_ref),
    )
    loads = [pltpu.make_async_copy(src, dst, load_sem.at[i]) for i, (src, dst) in enumerate(staged)]
    for load in loads:
        load.start()
    for load in loads:
        load.wait()
    for c in range(own):
        at = pl.ds(c * LANES, LANES)
        mine = pl.ds(0, rows)
        depth_ext[c, mine] = depth_ref[:, at]
        rain_ext[c, mine] = rain_ref[:, at]
        code = dir_ref[:, at]
        route = jnp.where(outlet_ref[:, at] == 1, 0, code + 1)
        route_ext[c, mine] = route
        far_ext[c, mine] = route
        coef_ext[c, mine] = conv_ref[:, at] * jnp.where(
            (code & 1) == 1, jnp.float32(0.70710678), jnp.float32(1.0)
        )
    def reach(index, peers):
        return 1 + jnp.where(index > 0, 1, 0) + jnp.where(index < peers - 1, 1, 0)

    pl.semaphore_wait(barrier, reach(my_row, row_peers) * reach(my_col, col_peers) - 1)

    firsts = (depth_ext, coef_ext, rain_ext, route_ext)
    far_slot, level_slot = (len(firsts), len(firsts) + 1)
    for slot, ext in enumerate(firsts):
        send(slot, ext, ext, NEAR)
    send(far_slot, far_ext, far_ext, MARGIN, slanted)
    unused = pl.ds(rows + NEAR, total - rows - 2 * NEAR)
    for ext in firsts:
        ext[:, unused] = jnp.zeros((own + 2, total - rows - 2 * NEAR, LANES), ext.dtype)
    if SPARE:
        for ext in (far_ext,) + tuple(acc_ext.at[g] for g in range(GROUPS)):
            ext[:, pl.ds(rows + MARGIN, SPARE)] = jnp.zeros((own + 2, SPARE, LANES), ext.dtype)
    for slot, ext in enumerate(firsts):
        receive(slot, ext, ext, NEAR)
    sides = (pl.ds(own, 2), pl.ds(0, rows))
    far_ext[sides] = route_ext[sides]

    right = lax.broadcasted_iota(jnp.int32, (SUB, LANES), 1) < LANES // 2

    def banded(ext, v):
        def part(c):
            return ext[c, pl.ds(v, SUB, stride=bands), :]

        blocks = [part(c) for c in range(own)]
        blocks.append(jnp.where(right, part(own), part(own + 1)))
        return jnp.concatenate(blocks, axis=1)

    for v in range(bands):
        acc[v] = banded(depth_ext, v)
        rain[v] = banded(rain_ext, v)
        coef[v] = banded(coef_ext, v)

    def above(v, get):
        return get(v - 1) if v else pltpu.roll(get(bands - 1), 1, 0)

    def below(v, get):
        return get(v + 1) if v < bands - 1 else pltpu.roll(get(0), SUB - 1, 0)

    def set_masks(ext):
        def routed(v):
            return banded(ext, v)

        for v in range(bands):
            near = {1: above(v, routed), 0: routed(v), -1: below(v, routed)}
            for k, (di, dj) in enumerate(OFFSETS):
                masks[k, v] = jnp.where(near[di] == k + 1, jnp.float32(1.0), jnp.float32(0.0))

    set_masks(route_ext)

    def inflow(v, up, here, down):
        near = {1: up, 0: here, -1: down}
        parts = {}
        for k, (di, dj) in enumerate(OFFSETS):
            term = masks[k, v] * near[di]
            parts[dj] = parts[dj] + term if dj in parts else term
        return parts[0] + (pltpu.roll(parts[1], 1, 1) + pltpu.roll(parts[-1], wide - 1, 1))

    def sweep(field, finish):
        start = field[0]
        up, here = (pltpu.roll(field[bands - 1], 1, 0), start)
        for v in range(bands):
            down = field[v + 1] if v < bands - 1 else pltpu.roll(start, SUB - 1, 0)
            finish(v, inflow(v, up, here, down))
            up, here = here, down

    @pl.loop(0, SUBSTEPS)
    def _(step):
        for v in range(bands):
            h = acc[v]
            factor = coef[v] * jnp.exp(jnp.log(h) * jnp.float32(2.0 / 3.0))
            out = h * (factor / (1.0 + factor))
            share[v] = out
            level[v] = h + rain[v] - out

        def finish(v, came):
            acc[v] = level[v] + came

        sweep(share, finish)

    def finish(v, came):
        acc[v] = level[v] + came

    def passes(count):
        @pl.loop(0, count)
        def _(index):
            sweep(acc, finish)

    def to_plain(field, dst):
        for v in range(bands):
            value = field[v]
            for c in range(own):
                dst[c, pl.ds(v, SUB, stride=bands), :] = value[:, c * LANES : (c + 1) * LANES]

    sub = lax.broadcasted_iota(jnp.int32, (SUB, LANES), 0)

    lane_part = lax.broadcasted_iota(jnp.int32, (SUB, LANES), 1) // MARGIN

    def corner(group, k):
        dr, dc = OFFSETS[k]
        slot = level_slot + group
        return pltpu.make_async_remote_copy(
            src_ref=pack_out.at[group, k],
            dst_ref=pack_in.at[group, k],
            send_sem=send_sem.at[slot, k],
            recv_sem=recv_sem.at[slot, k],
            device_id=(my_row + dr, my_col + dc),
            device_id_type=MESH,
        )

    def send_corners(group, src):
        for k in corners:
            dr, dc = OFFSETS[k]
            start = 0 if dr < 0 else rows - MARGIN
            block, first = (0, 0) if dc < 0 else (own - 1, LANES - MARGIN)
            packed = None
            for g in range(MARGIN // SUB):
                piece = src[block, pl.ds(start + g * SUB, SUB), :]
                shift = (g * MARGIN - first) % LANES
                piece = pltpu.roll(piece, shift, 1) if shift else piece
                packed = piece if packed is None else jnp.where(lane_part == g, piece, packed)
            pack_out[group, k] = packed
        for k in corners:
            @pl.when(exists(*OFFSETS[k]))
            def _(k=k):
                corner(group, k).start()

    def receive_corners(group, dst):
        for k in corners:
            dr, dc = OFFSETS[k]
            there = exists(-dr, -dc)
            start = rows if dr < 0 else total - MARGIN
            block, first = (own, 0) if dc < 0 else (own + 1, LANES - MARGIN)

            @pl.when(there)
            def _(k=k, start=start, block=block, first=first):
                corner(group, k).wait_recv()
                packed = pack_in[group, k]
                for g in range(MARGIN // SUB):
                    shift = (first - g * MARGIN) % LANES
                    piece = pltpu.roll(packed, shift, 1) if shift else packed
                    dst[block, pl.ds(start + g * SUB, SUB), :] = piece

            @pl.when(jnp.logical_not(there))
            def _(start=start, block=block):
                dst[block, pl.ds(start, MARGIN), :] = jnp.zeros((MARGIN, LANES), dst.dtype)

    def widen(src, dst, group, meanwhile, fields):
        slot = level_slot + group
        to_plain(acc, src)
        send_corners(group, src)
        send(slot, src, dst, MARGIN, straight)
        meanwhile()
        receive(slot, src, dst, MARGIN, straight)
        receive_corners(group, dst)
        for v in range(bands):
            inner = sub * bands + v < rows
            for c in range(own):
                at = pl.ds(c * LANES, LANES)
                value = jnp.where(inner, acc[v, :, at], dst[c, pl.ds(v, SUB, stride=bands), :])
                for field in fields:
                    field[v, :, at] = value
            value = jnp.where(
                right,
                dst[own, pl.ds(v, SUB, stride=bands), :],
                dst[own + 1, pl.ds(v, SUB, stride=bands), :],
            )
            for field in fields:
                field[v, :, pl.ds(cols, LANES)] = value

    def in_flight():
        for c in range(own):
            level_ref[:, pl.ds(c * LANES, LANES)] = plain[0, c, pl.ds(0, rows), :]
        receive(far_slot, far_ext, far_ext, MARGIN, slanted)
        set_masks(far_ext)

    widen(plain.at[0], acc_ext.at[0], 0, in_flight, (acc, level))
    passes(MARGIN)
    for group in range(1, GROUPS):
        widen(plain.at[group], acc_ext.at[group], group, lambda: None, (acc,))
        passes(MARGIN)

    to_plain(acc, plain.at[GROUPS])
    for c in range(own):
        discharge_ref[:, pl.ds(c * LANES, LANES)] = jnp.log(1.0 + plain[GROUPS, c, pl.ds(0, rows), :])
    for slot, ext in enumerate(firsts):
        sent_out(slot, ext, ext, NEAR)
    sent_out(far_slot, far_ext, far_ext, MARGIN, slanted)
    for group in range(GROUPS):
        sent_out(level_slot + group, plain.at[group], acc_ext.at[group], MARGIN, straight)
        for k in corners:
            @pl.when(exists(*OFFSETS[k]))
            def _(group=group, k=k):
                corner(group, k).wait_send()


def stage_plan():
    left, plan = PASSES, []
    for count in STAGES:
        plan.append((count, HALF - left, (LANES + 2 * left) // SUB))
        left -= count
    return plan


def strip_kernel(
    row_peers, col_peers,
    depth_hbm, rain_hbm, conv_hbm, dir_hbm, outlet_hbm,
    out_ref,
    conv_ref, dir_ref, outlet_ref,
    near, sides_in, rows_out, rows_in, corners_in, plain,
    h, rain, coef, base, share, near_masks,
    shifted, window,
    acc, level, hold, tall, moved, result,
    load_sem, near_send, near_recv, peer_send, peer_recv, rim_send, rim_recv,
    *stage_masks,
):
    rows, cols = conv_ref.shape
    own = cols // LANES
    total = plain.shape[1]
    thin = total // SUB
    east, west = own, own + 1
    wide = cols + 2 * LANES
    f32 = jnp.float32
    my_row, my_col = lax.axis_index("row"), lax.axis_index("col")

    def exists(dr, dc):
        r, c = my_row + dr, my_col + dc
        return (r >= 0) & (r < row_peers) & (c >= 0) & (c < col_peers)

    loads = [
        pltpu.make_async_copy(src, dst, load_sem.at[i])
        for i, (src, dst) in enumerate(
            [(conv_hbm, conv_ref), (dir_hbm, dir_ref), (outlet_hbm, outlet_ref)]
            + [
                (src.at[:, pl.ds(c * LANES, LANES)], near.at[a, c, pl.ds(0, rows)])
                for a, src in enumerate((depth_hbm, rain_hbm))
                for c in range(own)
            ]
        )
    ]
    for load in loads:
        load.start()
    barrier = pltpu.get_barrier_semaphore()

    def greet(row, col):
        pl.semaphore_signal(barrier, inc=1, device_id=(row, col), device_id_type=MESH)

    expected = row_peers - 1
    for dr, dc in OFFSETS:
        @pl.when(exists(dr, dc))
        def _(dr=dr, dc=dc):
            greet(my_row + dr, my_col + dc)
        if dc:
            expected = expected + jnp.where(exists(dr, dc), 1, 0)
    for q in range(row_peers):
        far = (my_row - q >= 2) | (q - my_row >= 2)

        @pl.when(far)
        def _(q=q):
            greet(q, my_col)

    for load in loads:
        load.wait()

    low = lax.broadcasted_iota(jnp.int32, (SUB, LANES), 1) < HALF

    for c in range(own):
        at = pl.ds(c * LANES, LANES)
        code = dir_ref[:, at]
        near[2, c, pl.ds(0, rows)] = conv_ref[:, at] * jnp.where(
            (code & 1) == 1, f32(0.70710678), f32(1.0)
        )
        near[3, c, pl.ds(0, rows)] = jnp.where(outlet_ref[:, at] == 1, 0, code + 1).astype(f32)

    for a in range(4):
        for c in range(own):
            at = pl.ds((c * 4 + a) * REACH, REACH)
            rows_out[0, at] = near[a, c, pl.ds(0, REACH)]
            rows_out[1, at] = near[a, c, pl.ds(rows - REACH, REACH)]

    every = range(rows // SUB)
    rim = (0, rows // SUB - 1)
    inner = range(1, rows // SUB - 1)

    def shift_tiles(field, get, blocks, tiles=every):
        for t in tiles:
            tile = pl.ds(t * SUB, SUB)
            turned = {}
            for j in blocks:
                for c in (j - 1, j):
                    if c not in turned:
                        turned[c] = pltpu.roll(get(west if c < 0 else c, tile), HALF, 1)
                shifted[field, j, tile] = jnp.where(low, turned[j - 1], turned[j])

    def route_tile(c, tile):
        return near[3, c, tile]

    def near_ends(k):
        dr, dc = OFFSETS[k]
        if dc == 0:
            part = pl.ds(0, 4 * own * REACH)
            src, dst = (
                (rows_out.at[0, part], rows_in.at[1, part])
                if dr < 0
                else (rows_out.at[1, part], rows_in.at[0, part])
            )
        elif dr == 0:
            part = pl.ds(0, rows)
            src = near.at[pl.ds(0, 3), 0 if dc < 0 else own - 1, part]
            dst = sides_in.at[0 if dc < 0 else 1, pl.ds(0, 3)]
        else:
            part = pl.ds(0 if dc < 0 else 4 * own * REACH - PACK, PACK)
            src = rows_out.at[0 if dr < 0 else 1, part]
            dst = corners_in.at[k, pl.ds(0, PACK)]
        return src, dst

    def near_copy(k):
        dr, dc = OFFSETS[k]
        src, dst = near_ends(k)
        return pltpu.make_async_remote_copy(
            src_ref=src, dst_ref=dst, send_sem=near_send.at[k], recv_sem=near_recv.at[k],
            device_id=(my_row + dr, my_col + dc), device_id_type=MESH,
        )

    def side_copy(side):
        return pltpu.make_async_remote_copy(
            src_ref=near.at[3, (0, own - 1)[side], pl.ds(0, rows)],
            dst_ref=sides_in.at[side, 3],
            send_sem=near_send.at[len(OFFSETS) + side], recv_sem=near_recv.at[len(OFFSETS) + side],
            device_id=(my_row, my_col + (-1, 1)[side]), device_id_type=MESH,
        )

    def window_copy(field, half, q):
        peer = lax.rem(my_row + q, row_peers)
        return pltpu.make_async_remote_copy(
            src_ref=shifted.at[field, peer + half],
            dst_ref=window.at[field, half, pl.ds(pl.multiple_of(my_row * rows, rows), rows)],
            send_sem=peer_send.at[field, half, q], recv_sem=peer_recv.at[field, half, q],
            device_id=(peer, my_col), device_id_type=MESH,
        )

    def part_copy(half, q, piece):
        peer = lax.rem(my_row + q, row_peers)
        start, size = ((SUB, rows - 2 * SUB), (0, SUB), (rows - SUB, SUB))[piece]
        send, recv = (peer_send, peer_recv) if piece == 0 else (rim_send, rim_recv)
        at = (1, half, q) if piece == 0 else (piece - 1, half, q)
        return pltpu.make_async_remote_copy(
            src_ref=shifted.at[1, peer + half, pl.ds(start, size)],
            dst_ref=window.at[1, half, pl.ds(pl.multiple_of(my_row * rows + start, SUB), size)],
            send_sem=send.at[at], recv_sem=recv.at[at],
            device_id=(peer, my_col), device_id_type=MESH,
        )

    def place(field):
        window[field, :, pl.ds(pl.multiple_of(my_row * rows, rows), rows)] = shifted[
            field, pl.ds(my_row, 2)
        ]

    def each(target, act):
        for q in range(1, row_peers):
            for half in (0, 1):
                row = lax.rem(my_row + q, row_peers) if target else my_row
                act(half, q, row == (0, row_peers - 1)[half])

    def send_route(late):
        def act(half, q, edge):
            @pl.when(edge if late else jnp.logical_not(edge))
            def _():
                window_copy(0, half, q).start()

        each(True, act)

    def send_inner():
        def act(half, q, edge):
            @pl.when(jnp.logical_not(edge))
            def _():
                part_copy(half, q, 0).start()

        each(True, act)

    def send_rest():
        def act(half, q, edge):
            @pl.when(edge)
            def _():
                window_copy(1, half, q).start()

            @pl.when(jnp.logical_not(edge))
            def _():
                part_copy(half, q, 1).start()
                part_copy(half, q, 2).start()

        each(True, act)

    def receive_level():
        def act(half, q, edge):
            @pl.when(edge)
            def _():
                window_copy(1, half, q).wait_recv()

            @pl.when(jnp.logical_not(edge))
            def _():
                for piece in range(3):
                    part_copy(half, q, piece).wait_recv()

        each(False, act)

    def level_sent():
        def act(half, q, edge):
            @pl.when(edge)
            def _():
                window_copy(1, half, q).wait_send()

            @pl.when(jnp.logical_not(edge))
            def _():
                for piece in range(3):
                    part_copy(half, q, piece).wait_send()

        each(True, act)

    def receive_window(field):
        for q in range(1, row_peers):
            for half in (0, 1):
                window_copy(field, half, q).wait_recv()

    def window_sent(field):
        for q in range(1, row_peers):
            for half in (0, 1):
                window_copy(field, half, q).wait_send()

    order = (1, 3, 5, 7, 2, 6, 0, 4)
    pl.semaphore_wait(barrier, expected)
    for side, dc in enumerate((-1, 1)):
        @pl.when(exists(0, dc))
        def _(side=side):
            side_copy(side).start()
    for k in order:
        @pl.when(exists(*OFFSETS[k]))
        def _(k=k):
            near_copy(k).start()
    shift_tiles(0, route_tile, range(1, own))
    send_route(False)

    near[:, pl.ds(0, own), pl.ds(rows, total - rows)] = jnp.zeros((4, own, total - rows, LANES), f32)
    near[:, pl.ds(own, 2), pl.ds(0, total)] = jnp.zeros((4, 2, total, LANES), f32)

    def near_band(a, v):
        take = pl.ds(v, SUB, stride=thin)
        return jnp.concatenate([near[a, c, take, :] for c in range(own + 2)], axis=1)

    def mask_rows(dst, count, up, here, down):
        for v in range(count):
            rows_near = {1: up(v), 0: here(v), -1: down(v)}
            for k, (di, dj) in enumerate(OFFSETS):
                dst[k, v] = jnp.where(rows_near[di] == k + 1, f32(1.0), f32(0.0))

    def sweep(field, mask, count, width, finish):
        start = field[0]
        up, here = pltpu.roll(field[count - 1], 1, 0), start
        for v in range(count):
            down = field[v + 1] if v < count - 1 else pltpu.roll(start, SUB - 1, 0)
            rows_near = {1: up, 0: here, -1: down}
            parts = {}
            for k, (di, dj) in enumerate(OFFSETS):
                term = mask[k, v] * rows_near[di]
                parts[dj] = parts[dj] + term if dj in parts else term
            finish(
                v, parts[0] + (pltpu.roll(parts[1], 1, 1) + pltpu.roll(parts[-1], width - 1, 1))
            )
            up, here = here, down

    def levels():
        for v in range(thin):
            h[v] = near_band(0, v)
            rain[v] = near_band(1, v)
            coef[v] = near_band(2, v)
            base[v] = near_band(3, v)

        mask_rows(
            near_masks, thin,
            lambda v: base[v - 1] if v else pltpu.roll(base[thin - 1], 1, 0),
            lambda v: base[v],
            lambda v: base[v + 1] if v < thin - 1 else pltpu.roll(base[0], SUB - 1, 0),
        )

        @pl.loop(0, SUBSTEPS)
        def _(step):
            for v in range(thin):
                depth = h[v]
                factor = coef[v] * jnp.exp(jnp.log(depth) * f32(2.0 / 3.0))
                out = depth * (factor / (1.0 + factor))
                share[v] = out
                base[v] = depth + rain[v] - out

            def finish(v, came):
                h[v] = base[v] + came

            sweep(share, near_masks, thin, wide, finish)

        for v in range(thin):
            value = h[v]
            for c in range(own + 2):
                plain[c, pl.ds(v, SUB, stride=thin), :] = value[:, c * LANES : (c + 1) * LANES]

    def level_tile(c, tile):
        return plain[c, tile]

    levels()
    shift_tiles(1, level_tile, range(1, own), inner)
    send_inner()
    for side, dc in enumerate((-1, 1)):
        there = exists(0, -dc)

        @pl.when(there)
        def _(side=side):
            side_copy(side).wait_recv()

        @pl.when(jnp.logical_not(there))
        def _(side=side):
            sides_in[side, 3] = jnp.zeros((rows, LANES), f32)

        near[3, own + side, pl.ds(0, rows)] = sides_in[side, 3]
    shift_tiles(0, route_tile, (0, own))
    send_route(True)
    place(0)
    for k in order:
        dr, dc = OFFSETS[k]
        there = exists(-dr, -dc)

        @pl.when(there)
        def _(k=k):
            near_copy(k).wait_recv()

        @pl.when(jnp.logical_not(there))
        def _(k=k):
            dst = near_ends(k)[1]
            dst[...] = jnp.zeros(dst.shape, f32)

    below, above = pl.ds(rows, REACH), pl.ds(total - REACH, REACH)
    for a in range(4):
        for c in range(own):
            at = pl.ds((c * 4 + a) * REACH, REACH)
            near[a, c, below] = rows_in[1, at]
            near[a, c, above] = rows_in[0, at]
        for k in (1, 3, 5, 7):
            dr, dc = OFFSETS[k]
            start = 0 if dc < 0 else PACK - 4 * REACH
            near[a, east if dc < 0 else west, below if dr < 0 else above] = corners_in[
                k, pl.ds(start + a * REACH, REACH)
            ]

    for side in (0, 1):
        near[pl.ds(0, 3), own + side, pl.ds(0, rows)] = sides_in[side, pl.ds(0, 3)]

    levels()
    shift_tiles(1, level_tile, (0, own))
    shift_tiles(1, level_tile, range(1, own), rim)
    send_rest()
    place(1)
    for c in range(own):
        out_ref[0, :, pl.ds(c * LANES, LANES)] = plain[c, pl.ds(0, rows)]

    def lay(field):
        for b in (0, 1):
            for half in (0, 1):
                tall[b, pl.ds(half * LANES, LANES), :] = window[
                    field, half, pl.ds(b, LANES, stride=2), :
                ].T

    def band(ref, first, count, v, b):
        return ref[b, pl.ds(first + v, SUB, stride=count), :]

    plan = stage_plan()
    along = lax.broadcasted_iota(jnp.int32, (SUB, LANES), 1)
    receive_window(0)
    lay(0)
    for (_, first, count), masks in zip(plan, stage_masks):
        for b in (0, 1):
            codes = [band(tall, first, count, v, b) for v in range(count)]
            for v in range(count):
                cols_near = {
                    1: codes[v - 1] if v else pltpu.roll(codes[-1], 1, 0),
                    0: codes[v],
                    -1: codes[v + 1] if v < count - 1 else pltpu.roll(codes[0], SUB - 1, 0),
                }
                for k, (di, dj) in enumerate(OFFSETS):
                    here = cols_near[dj] == k + 1
                    if (di, b) == (1, 1):
                        here = here & (along < LANES - 1)
                    elif (di, b) == (-1, 0):
                        here = here & (along > 0)
                    masks[k, v, b] = jnp.where(here, f32(1.0), f32(0.0))
    receive_level()
    lay(1)

    def pair(ref, v):
        return ref[v, 0], ref[v, 1]

    def turn(values, amount):
        return tuple(pltpu.roll(value, amount, 0) for value in values)

    def gather(held, seed, left, here, right):
        cols_near = {1: left, 0: here, -1: right}
        parts = {}
        for k, (di, dj) in enumerate(OFFSETS):
            for b in (0, 1):
                term = held[k, b] * cols_near[dj][b]
                parts[di, b] = parts[di, b] + term if (di, b) in parts else term
        return (
            seed[0] + (parts[0, 0] + (parts[-1, 1] + pltpu.roll(parts[1, 1], 1, 1))),
            seed[1] + (parts[0, 1] + (parts[1, 0] + pltpu.roll(parts[-1, 0], LANES - 1, 1))),
        )

    def put(ref, v, values):
        ref[v, 0], ref[v, 1] = values

    def run(passes, masks, count):
        def fetch(v):
            return {(k, b): masks[k, v, b] for k in range(len(OFFSETS)) for b in (0, 1)}

        @pl.loop(0, passes // 2)
        def _(index):
            last = count - 1
            first = pair(acc, 0)
            edge = gather(
                fetch(last), pair(level, last), pair(acc, last - 1), pair(acc, last),
                turn(first, SUB - 1),
            )
            put(hold, 2, edge)
            left, here = turn(pair(acc, last), 1), first
            older = newer = held = seed = None
            for v in range(last):
                right = pair(acc, v + 1)
                fresh, start = fetch(v), pair(level, v)
                value = gather(fresh, start, left, here, right)
                if v < 2:
                    put(hold, v, value)
                else:
                    put(acc, v - 1, gather(held, seed, older, newer, value))
                older, newer = newer, value
                held, seed = fresh, start
                left, here = here, right
            edge = pair(hold, 2)
            put(acc, last - 1, gather(held, seed, older, newer, edge))
            put(
                acc, last,
                gather(fetch(last), pair(level, last), newer, edge, turn(pair(hold, 0), SUB - 1)),
            )
            put(
                acc, 0,
                gather(fetch(0), pair(level, 0), turn(edge, 1), pair(hold, 0), pair(hold, 1)),
            )

    source = tall
    for (passes, first, count), masks in zip(plan, stage_masks):
        for v in range(count):
            for b in (0, 1):
                value = band(tall, first, count, v, b)
                level[v, b] = value
                acc[v, b] = value if source is tall else band(source, first, count, v, b)
        run(passes, masks, count)
        source = moved
        for v in range(count):
            for b in (0, 1):
                moved[b, pl.ds(first + v, SUB, stride=count), :] = acc[v, b]
    for b in (0, 1):
        core = jnp.log(1.0 + moved[b, pl.ds(HALF, LANES), :])
        result[pl.ds(b, LANES, stride=2), :] = core.T

    mine = pl.ds(pl.multiple_of(my_row * LANES, LANES), LANES)

    def result_copy(q):
        peer = lax.rem(my_row + q, row_peers)
        return pltpu.make_async_remote_copy(
            src_ref=result.at[pl.ds(pl.multiple_of(peer * rows, rows), rows)],
            dst_ref=out_ref.at[1, :, mine],
            send_sem=peer_send.at[2, 0, q], recv_sem=peer_recv.at[2, 0, q],
            device_id=(peer, my_col), device_id_type=MESH,
        )

    for q in range(1, row_peers):
        result_copy(q).start()
    out_ref[1, :, mine] = result[pl.ds(pl.multiple_of(my_row * rows, rows), rows)]
    for k in order:
        @pl.when(exists(*OFFSETS[k]))
        def _(k=k):
            near_copy(k).wait_send()
    for side, dc in enumerate((-1, 1)):
        @pl.when(exists(0, dc))
        def _(side=side):
            side_copy(side).wait_send()
    window_sent(0)
    level_sent()
    for q in range(1, row_peers):
        result_copy(q).wait_recv()
    for q in range(1, row_peers):
        result_copy(q).wait_send()


def strip_call(row_peers, col_peers, rows, cols):
    own = cols // LANES
    total = rows + 2 * SUB
    thin, bands = total // SUB, 2 * LANES // SUB
    f32, i32 = jnp.float32, jnp.int32
    tile = (rows, cols)
    slim = (thin, SUB, cols + 2 * LANES)
    field = (bands, 2, SUB, LANES)
    return pl.pallas_call(
        functools.partial(strip_kernel, row_peers, col_peers),
        out_shape=jax.ShapeDtypeStruct((2, rows, cols), f32),
        in_specs=[pl.BlockSpec(memory_space=pltpu.HBM)] * 5,
        out_specs=pl.BlockSpec(memory_space=pltpu.VMEM),
        scratch_shapes=[
            pltpu.VMEM(tile, f32),
            pltpu.VMEM(tile, i32),
            pltpu.VMEM(tile, i32),
            pltpu.VMEM((4, own + 2, total + SUB, LANES), f32),
            pltpu.VMEM((2, 4, rows, LANES), f32),
            pltpu.VMEM((2, 4 * own * REACH + SUB, LANES), f32),
            pltpu.VMEM((2, 4 * own * REACH + SUB, LANES), f32),
            pltpu.VMEM((len(OFFSETS), PACK + SUB, LANES), f32),
            pltpu.VMEM((own + 2, total, LANES), f32),
            pltpu.VMEM(slim, f32),
            pltpu.VMEM(slim, f32),
            pltpu.VMEM(slim, f32),
            pltpu.VMEM(slim, f32),
            pltpu.VMEM(slim, f32),
            pltpu.VMEM((len(OFFSETS),) + slim, f32),
            pltpu.VMEM((2, own + 1, rows, LANES), f32),
            pltpu.VMEM((2, 2, row_peers * rows, LANES), f32),
            pltpu.VMEM(field, f32),
            pltpu.VMEM(field, f32),
            pltpu.VMEM((3, 2, SUB, LANES), f32),
            pltpu.VMEM((2, 2 * LANES, LANES), f32),
            pltpu.VMEM((2, 2 * LANES, LANES), f32),
            pltpu.VMEM((row_peers * rows, LANES), f32),
            pltpu.SemaphoreType.DMA((3 + 2 * own,)),
            pltpu.SemaphoreType.DMA((len(OFFSETS) + 2,)),
            pltpu.SemaphoreType.DMA((len(OFFSETS) + 2,)),
            pltpu.SemaphoreType.DMA((3, 2, row_peers)),
            pltpu.SemaphoreType.DMA((3, 2, row_peers)),
            pltpu.SemaphoreType.DMA((2, 2, row_peers)),
            pltpu.SemaphoreType.DMA((2, 2, row_peers)),
        ]
        + [
            pltpu.VMEM((len(OFFSETS), count, 2, SUB, LANES), f32)
            for _, _, count in stage_plan()
        ],
        compiler_params=pltpu.CompilerParams(
            collective_id=0, has_side_effects=True, vmem_limit_bytes=VMEM_BYTES
        ),
    )


def solution(mesh):
    row_peers, col_peers = mesh.shape["row"], mesh.shape["col"]

    def on_device(depth, rainfall, conveyance, flow_dir, outlet):
        rows, cols = depth.shape
        total = rows + 2 * MARGIN + SPARE
        bands = total // SUB
        wide = cols + LANES
        slots = 5 + GROUPS
        own = cols // LANES
        ext = (own + 2, total, LANES)
        field = (bands, SUB, wide)
        vmem = pl.BlockSpec(memory_space=pltpu.VMEM)
        f32 = jnp.float32
        args = tuple(
            pltpu.with_memory_space_constraint(a, pltpu.HBM)
            for a in (depth, rainfall, conveyance, flow_dir, outlet)
        )
        strips = row_peers > 1 and cols == row_peers * LANES and row_peers * rows == 2 * LANES
        if strips and rows % PACK == 0 and row_peers % 2 == 0:
            both = strip_call(row_peers, col_peers, rows, cols)(*args)
            return both[0], both[1]
        hbm = pl.BlockSpec(memory_space=pltpu.HBM)
        tile = (rows, cols)
        both = pl.pallas_call(
            functools.partial(kernel, row_peers, col_peers),
            out_shape=jax.ShapeDtypeStruct((2, rows, cols), f32),
            in_specs=[hbm] * 5,
            out_specs=vmem,
            scratch_shapes=[
                pltpu.VMEM(tile, f32),
                pltpu.VMEM(tile, f32),
                pltpu.VMEM(tile, f32),
                pltpu.VMEM(tile, jnp.int32),
                pltpu.VMEM(tile, jnp.int32),
                pltpu.SemaphoreType.DMA((5,)),
                pltpu.VMEM(ext, f32),
                pltpu.VMEM(ext, f32),
                pltpu.VMEM(ext, f32),
                pltpu.VMEM(ext, jnp.int32),
                pltpu.VMEM(ext, jnp.int32),
                pltpu.VMEM((GROUPS,) + ext, f32),
                pltpu.VMEM((GROUPS + 1, own, total, LANES), f32),
                pltpu.VMEM((GROUPS, len(OFFSETS), SUB, LANES), f32),
                pltpu.VMEM((GROUPS, len(OFFSETS), SUB, LANES), f32),
                pltpu.VMEM(field, f32),
                pltpu.VMEM(field, f32),
                pltpu.VMEM(field, f32),
                pltpu.VMEM(field, f32),
                pltpu.VMEM(field, f32),
                pltpu.VMEM((len(OFFSETS),) + field, f32),
                pltpu.SemaphoreType.DMA((slots, len(OFFSETS))),
                pltpu.SemaphoreType.DMA((slots, len(OFFSETS))),
            ],
            compiler_params=pltpu.CompilerParams(
                collective_id=0, has_side_effects=True, vmem_limit_bytes=VMEM_BYTES
            ),
        )(*args)
        return both[0], both[1]

    placed = P("row", "col")
    return jax.shard_map(
        on_device,
        mesh=mesh,
        in_specs=(placed,) * 5,
        out_specs=(placed, placed),
        check_vma=False,
    )
```
